32 devices in a mesh: seq: 8 (over z, core), fsdp: 4 (over y, x).
Axes of the slice: x: 2, y: 2, z: 4, core: 2. Of those that a mesh axis runs over, the one named last changes fastest.
Arguments:
- patches: bfloat16 [4, 1024, 3072], P('fsdp', 'seq'), may hold values from -6 to 6
- weight_codes: int32 [3072, 3072], P('fsdp'), may hold values from -448 to 448
- block_scales: float32 [24, 24], P('fsdp'), may hold values from 2.5e-05 to 0.0001
- key_proj: bfloat16 [4, 1024, 3072], P('fsdp', 'seq'), may hold values from -6 to 6
- value_proj: bfloat16 [4, 1024, 3072], P('fsdp', 'seq'), may hold values from -6 to 6
- query_gain: float32 [3072], replicated, may hold values from 1 to 10
- key_gain: float32 [3072], replicated, may hold values from 1 to 10
Outputs:
- attended: bfloat16 [4, 1024, 3072], P('fsdp', 'seq')
The draws below stay inside these ranges and needn't reach their ends.
All inputs are finite; a program needn't handle non-finite values.
Results may differ from the reference program's by a relative error of at most 0.007.
The reference program's roundings to bfloat16 on the way count: a program that leaves them out, or rounds other values in their place, can miss the bound.
Values may be sent and summed in bfloat16 or wider, within the bound.
A program may use at most 192 MiB of HBM per device.

```python
import math
import jax
import jax.numpy as jnp
from jax import lax

D = 3072
HEADS = 48
HDIM = 64
BLOCK = 128
IMAGES = 4
SEQ = 1024


def gain_values(key, which):
    own_key = jax.random.fold_in(key, which)
    values = jnp.exp(jax.random.uniform(own_key, (HEADS, HDIM), minval=0.0, maxval=math.log(3.0)))
    return values.reshape(HEADS * HDIM).astype(jnp.float32)


def draw_query_gain(key, part):
    return gain_values(key, 1)


def draw_key_gain(key, part):
    return gain_values(key, 2)


def touch_ends(drawn, rng, least, high):
    index_at = [jax.random.randint(jax.random.fold_in(rng, axis), (), 0, length) for axis, length in enumerate(drawn.shape)]
    longest = drawn.shape.index(max(drawn.shape))
    next_to = index_at[:longest] + [(index_at[longest] + 1) % drawn.shape[longest]] + index_at[longest + 1:]
    return drawn.at[tuple(index_at)].set(least).at[tuple(next_to)].set(high)


def block_scale(key, dims, pieces, smallest, high):
    gain, own = 1.0, jax.random.fold_in(key, 6)
    for dim, shards_of in pieces:
        steps = jnp.exp(jax.random.uniform(jax.random.fold_in(own, dim), (shards_of,), jnp.float32, smallest / len(pieces), high / len(pieces)))
        gain = gain * jnp.repeat(steps, dims[dim] // shards_of).reshape([-1 if axis == dim else 1 for axis in range(len(dims))])
    return gain


def bell_draw(key, shape, deviation, limit, shards=(), held_as=jnp.bfloat16):
    values = deviation * jax.random.normal(key, shape, jnp.float32)
    if shards:
        values = values * block_scale(key, shape, shards, -0.22, 0.18)
    return jnp.clip(values, -limit, limit).astype(held_as)


def setup_inputs(seed: int = 0) -> dict:
    keys = jax.random.split(jax.random.key(seed), 8)
    return {
        "patches": bell_draw(keys[0], (IMAGES, SEQ, D), 1.0, 6.0, ((0, 4), (1, 8))),
        "weight_codes": touch_ends(jax.random.randint(keys[1], (D, HEADS * HDIM), -448, 449), jax.random.fold_in(keys[1], 1), -448, 448).astype(jnp.int32),
        "block_scales": jnp.clip(jnp.exp(math.log(0.0001) - 1.3862944 * jax.random.uniform(keys[2], (D // BLOCK, HEADS * HDIM // BLOCK), jnp.float32) ** block_scale(keys[2], (D // BLOCK, HEADS * HDIM // BLOCK), ((0, 4),), -0.2, 0.2)), 2.499999936844688e-05, 0.0001),
        "key_proj": bell_draw(keys[3], (IMAGES, SEQ, HEADS * HDIM), 1.0, 6.0, ((0, 4), (1, 8))),
        "value_proj": bell_draw(keys[4], (IMAGES, SEQ, HEADS * HDIM), 1.0, 6.0, ((0, 4), (1, 8))),
        "query_gain": draw_query_gain(jax.random.fold_in(keys[7], 71), 0),
        "key_gain": draw_key_gain(jax.random.fold_in(keys[7], 71), 0),
    }


NORM_FLOOR = 0.25

def head_norm(projected, gain_row):
    shaped = projected.reshape(projected.shape[:-1] + (HEADS, HDIM))
    average = lax.optimization_barrier(jnp.mean(shaped, axis=-1, keepdims=True))
    centred = shaped - average
    spread = lax.optimization_barrier(jnp.mean(centred * centred, axis=-1, keepdims=True))
    normed = centred * lax.rsqrt(spread + NORM_FLOOR) * gain_row.reshape(HEADS, HDIM)
    return normed.astype(jnp.bfloat16)

def reference(patches, weight_codes, block_scales, key_proj, value_proj, query_gain, key_gain):
    column_count = HEADS * HDIM
    blocked = weight_codes.astype(jnp.float32).reshape(D // BLOCK, BLOCK, column_count // BLOCK, BLOCK)
    weight = (blocked * block_scales[:, None, :, None]).reshape(D, column_count).astype(jnp.bfloat16)
    queries = jnp.dot(patches.reshape(IMAGES * SEQ, D), weight, preferred_element_type=jnp.float32)
    queries = queries.reshape(IMAGES, SEQ, column_count)
    query_view = head_norm(queries, query_gain)
    key_view = head_norm(key_proj.astype(jnp.float32), key_gain)
    value_view = value_proj.reshape(IMAGES, SEQ, HEADS, HDIM)

    def one_head(members):
        query_head, key_head, value_head = members
        scores = jnp.einsum('iqd,ikd->iqk', query_head.astype(jnp.float32), key_head.astype(jnp.float32)) * HDIM ** (-0.5)
        largest = lax.optimization_barrier(jnp.max(scores, axis=-1, keepdims=True))
        probability = jnp.exp(scores - largest)
        normaliser = lax.optimization_barrier(jnp.sum(probability, axis=-1))
        rounded = lax.optimization_barrier(probability.astype(jnp.bfloat16))
        blended = jnp.einsum('iqk,ikd->iqd', rounded.astype(jnp.float32), value_head.astype(jnp.float32))
        return blended / normaliser[..., None]
    outputs = lax.map(one_head, (jnp.moveaxis(query_view, 2, 0), jnp.moveaxis(key_view, 2, 0), jnp.moveaxis(value_view, 2, 0)))
    return jnp.moveaxis(outputs, 0, 2).reshape(IMAGES, SEQ, column_count).astype(jnp.bfloat16)
```

```python
import functools
import math
import jax
import jax.numpy as jnp
from jax import lax
from jax.experimental import pallas as pl
from jax.experimental.pallas import tpu as pltpu
from jax.sharding import PartitionSpec as P

HEADS = 48
HDIM = 64
BLOCK = 128


NORM_FLOOR = 0.25


def head_norm(projected, gain_row):
    shaped = projected.reshape(projected.shape[:-1] + (HEADS, HDIM))
    average = jnp.mean(shaped, axis=-1, keepdims=True)
    centred = shaped - average
    spread = jnp.mean(centred * centred, axis=-1, keepdims=True)
    normed = centred * lax.rsqrt(spread + NORM_FLOOR) * gain_row.reshape(HEADS, HDIM)
    return normed.astype(jnp.bfloat16)


def dequantize(weight_codes, block_scales):
    row_count, column_count = weight_codes.shape
    blocked = weight_codes.astype(jnp.float32).reshape(
        row_count // BLOCK, BLOCK, column_count // BLOCK, BLOCK
    )
    return (
        (blocked * block_scales[:, None, :, None])
        .reshape(row_count, column_count)
        .astype(jnp.bfloat16)
    )


def start_of(query_view):
    image_count, token_count, head_count = (
        query_view.shape[0],
        query_view.shape[1],
        query_view.shape[2],
    )
    return (
        jnp.full((image_count, token_count, head_count), -1e30, jnp.float32),
        jnp.zeros((image_count, token_count, head_count), jnp.float32),
        jnp.zeros(query_view.shape, jnp.float32),
    )


def attend_block(query_view, state_now, key_view, value_view):
    running_max, running_sum, weighted = state_now
    scores = jnp.einsum(
        "ithd,ishd->iths", query_view, key_view, preferred_element_type=jnp.float32
    ) * HDIM ** (-0.5)
    newest = jnp.maximum(running_max, jnp.max(scores, axis=-1))
    probability = jnp.exp(scores - newest[..., None])
    running_sum = jnp.sum(probability, axis=-1)
    blended = jnp.einsum(
        "iths,ishd->ithd",
        probability.astype(jnp.bfloat16),
        value_view,
        preferred_element_type=jnp.float32,
    )
    weighted = blended
    return (newest, running_sum, weighted)


def per_device(patches, weight_codes, block_scales, key_proj, value_proj, query_gain, key_gain):
    image_count, token_count, feature_count = patches.shape
    flat_rows = patches.reshape(image_count * token_count, feature_count)
    key_norm = head_norm(key_proj.astype(jnp.float32), key_gain)
    value_view = value_proj.reshape(image_count, token_count, HEADS, HDIM)
    local_weight = dequantize(weight_codes, block_scales)
    group_rows = lax.all_to_all(flat_rows, "fsdp", split_axis=1, concat_axis=0, tiled=True)
    queries = lax.psum_scatter(
        jnp.dot(group_rows, local_weight, preferred_element_type=jnp.float32),
        "fsdp",
        scatter_dimension=0,
        tiled=True,
    )
    query_view = head_norm(queries, query_gain).reshape(image_count, token_count, HEADS, HDIM)
    finished = attend_block(
        query_view,
        start_of(query_view),
        lax.all_gather(key_norm, "seq", axis=1, tiled=True),
        lax.all_gather(value_view, "seq", axis=1, tiled=True),
    )
    attended = finished[2] / finished[1][..., None]
    return attended.reshape(image_count, token_count, HEADS * HDIM).astype(jnp.bfloat16)


MESH = pl.DeviceIdType.MESH
LANES = 128
CORES = 2
GRID = 2


def column_norm(values, gain_row):
    lane = lambda axis: lax.broadcasted_iota(jnp.int32, (LANES, LANES), axis) < HDIM
    spread_out = jnp.where(lane(0) == lane(1), 1.0 / HDIM, 0.0).astype(jnp.bfloat16)
    spread_out = jnp.concatenate([spread_out, spread_out], axis=0)

    def mean_of(t):
        high = t.astype(jnp.bfloat16)
        low = (t - high.astype(jnp.float32)).astype(jnp.bfloat16)
        return jnp.dot(jnp.concatenate([high, low], axis=1), spread_out, preferred_element_type=jnp.float32)

    centred = values - mean_of(values)
    normed = centred * lax.rsqrt(mean_of(centred * centred) + NORM_FLOOR) * gain_row
    return normed.astype(jnp.bfloat16)


def fused_kernel(
    n, fn, patches, codes, scales_in, key, value, query_gain_in, key_gain_in, out,
    pbuf, cbuf, wbuf, kv, qsend, qbuf, obuf, gains, scales,
    code_sem, scale_sem, gain_sem, mate_recv, rest_recv, p_send, near_recv, relay_recv, w_send,
    kv_send, kv_recv, q_send, q_recv, o_send, o_recv,
):
    s, f = lax.axis_index("seq"), lax.axis_index("fsdp")
    m = n // 2
    half, place = s // m, lax.rem(s, m)
    tokens = patches.shape[0]
    rows, columns = codes.shape
    width = columns // n
    chunks = width // LANES
    group = m * tokens
    chips = m // CORES
    core = lax.rem(s, CORES)
    partner = s + 1 - 2 * core

    barrier = pltpu.get_barrier_semaphore()
    for d in range(1, n):
        pl.semaphore_signal(barrier, inc=1, device_id={"seq": lax.rem(s + d, n)}, device_id_type=MESH)
    for d in range(1, fn):
        pl.semaphore_signal(barrier, inc=1, device_id={"fsdp": lax.rem(f + d, fn)}, device_id_type=MESH)

    def chip_mate(d):
        return half * m + lax.rem(place + d * CORES, m)

    def rows_of(device):
        return pl.ds(pl.multiple_of(lax.rem(device, m) * tokens, tokens), tokens)

    def all_rows_of(device):
        return pl.ds(pl.multiple_of(device * tokens, tokens), tokens)

    def owned(device):
        return pl.multiple_of((lax.rem(device, m) * 2 + device // m) * width, LANES)

    def owned_chunk(device, k):
        return pl.ds(pl.multiple_of(owned(device) + k * LANES, LANES), LANES)

    def chunk_column(q):
        side = jnp.where(q < chunks, 1 - half, half)
        return pl.multiple_of((place * 2 + side) * width + lax.rem(q, chunks) * LANES, LANES)

    def drain(ref, sem):
        pltpu.make_async_copy(ref, ref, sem).wait()

    pltpu.make_async_copy(scales_in, scales, scale_sem.at[0]).start()
    for q in range(2 * chunks):
        pltpu.make_async_copy(codes.at[:, pl.ds(chunk_column(q), LANES)], cbuf.at[q], code_sem.at[0]).start()
    pltpu.make_async_copy(patches, pbuf.at[rows_of(s)], rest_recv.at[0]).start()
    pltpu.make_async_copy(query_gain_in, gains.at[0], gain_sem.at[0]).start()
    pltpu.make_async_copy(key_gain_in, gains.at[1], gain_sem.at[0]).start()
    for k in range(chunks):
        for which, src in enumerate((key, value)):
            pltpu.make_async_copy(
                src.at[:, owned_chunk(s, k)], kv.at[k, which, all_rows_of(s)], kv_recv.at[k]).start()

    pl.semaphore_wait(barrier, n - 1 + fn - 1)

    def remote(src, dst, send, recv, **device):
        return pltpu.make_async_remote_copy(
            src_ref=src, dst_ref=dst, send_sem=send, recv_sem=recv, device_id=device, device_id_type=MESH)

    def mate_copy(d):
        return remote(patches, pbuf.at[rows_of(s)], p_send.at[0], mate_recv.at[d - 1], seq=chip_mate(d))

    for d in range(1, chips):
        mate_copy(d).start()

    far = place // CORES == jnp.where(half == 0, 0, chips - 1)

    def start_kv(to):
        def one(k, _):
            for which, src in enumerate((key, value)):
                remote(
                    src.at[:, owned_chunk(to, k)], kv.at[k, which, all_rows_of(s)],
                    kv_send.at[0], kv_recv.at[k], seq=to).start()
            return 0

        return one

    def kv_across():
        for j in range(chips):
            chip = jnp.where(half == 0, chips + j, chips - 1 - j)

            def both(k, _):
                for c in range(CORES):
                    start_kv(chip * CORES + c)(k, 0)
                return 0

            lax.fori_loop(0, chunks, both, 0)

    def kv_beside():
        for d in range(1, chips):
            chip = chip_mate(d) // CORES

            def both(k, _):
                for c in range(CORES):
                    start_kv(chip * CORES + c)(k, 0)
                return 0

            lax.fori_loop(0, chunks, both, 0)

    kv_across()
    remote(patches, pbuf.at[rows_of(s)], p_send.at[0], rest_recv.at[0], seq=partner).start()
    lax.fori_loop(0, chunks, start_kv(partner), 0)
    pl.when(jnp.logical_not(far))(kv_beside)

    row_mate = f + 1 - 2 * lax.rem(f, GRID)
    column_mate = lax.rem(f + GRID, fn)

    def weight_copy(pair, recv, start, size, to):
        at = pl.ds(pl.multiple_of(start, size), size)
        return remote(wbuf.at[pair, at], wbuf.at[pair, at], w_send.at[0], recv.at[pair], fsdp=to)

    def near_start(pair):
        weight_copy(pair, near_recv, f * rows, rows, row_mate).start()
        weight_copy(pair, near_recv, f * rows, rows, column_mate).start()

    def relay(pair):
        part = rows // 2
        drain(wbuf.at[pair, pl.ds(0, 2 * rows)], near_recv.at[pair])
        weight_copy(pair, relay_recv, row_mate * rows, part, column_mate).start()
        weight_copy(pair, relay_recv, column_mate * rows + part, part, row_mate).start()

    drain(scales, scale_sem.at[0])
    drain(cbuf, code_sem.at[0])

    def dequantize_pair(pair, _):
        for side in range(2):
            q = 2 * pair + side
            for block in range(rows // BLOCK):
                scale = scales[block, chunk_column(q) // BLOCK]
                piece = cbuf[q, block * BLOCK:(block + 1) * BLOCK, :].astype(jnp.float32) * scale
                at = pl.ds(pl.multiple_of(f * rows + block * BLOCK, BLOCK), BLOCK)
                wbuf[pair, at, side * LANES:(side + 1) * LANES] = piece.astype(jnp.bfloat16)

        @pl.when(pair < chunks - 1)
        def _():
            near_start(pair)

        return 0

    lax.fori_loop(0, chunks, dequantize_pair, 0)

    for pair in range(chunks - 1):
        relay(pair)
    near_start(chunks - 1)

    for d in range(1, chips):
        at = rows_of(half * m + lax.rem(place + m - d * CORES, m))
        drain(pbuf.at[at], mate_recv.at[d - 1])
        remote(pbuf.at[at], pbuf.at[at], p_send.at[0], rest_recv.at[0], seq=partner).start()
    drain(gains, gain_sem.at[0])
    drain(pbuf.at[pl.ds(0, (chips + 1) * tokens)], rest_recv.at[0])

    other = lax.rem(s + m, n)
    half_rows = pl.ds(pl.multiple_of(half * group, group), group)

    def query_copy(k):
        return remote(qsend.at[k], qbuf.at[k, half_rows], q_send.at[0], q_recv.at[k], seq=other)

    def project(pair):
        drain(wbuf.at[pair, pl.ds(0, rows)], relay_recv.at[pair])
        both = jnp.dot(pbuf[...], wbuf[pair], preferred_element_type=jnp.float32)
        for side in range(2):
            q = 2 * pair + side
            normed = column_norm(
                both[:, side * LANES:(side + 1) * LANES], gains[0, :, pl.ds(chunk_column(q), LANES)])
            if q < chunks:
                qsend[q] = normed
                query_copy(q).start()
            else:
                qbuf[q - chunks, half_rows] = normed

    for pair in range(chunks - 1):
        project(pair)
    pl.when(far)(kv_beside)
    relay(chunks - 1)
    project(chunks - 1)

    tile = CORES * tokens
    exponent = HDIM ** (-0.5) * math.log2(math.e)

    def out_copy(k, to):
        return remote(obuf.at[k, all_rows_of(to)], out.at[:, owned_chunk(s, k)], o_send.at[0], o_recv.at[0], seq=to)

    first = lax.broadcasted_iota(jnp.int32, (tile, LANES), 1) < HDIM
    last = 2 * chunks - 1

    def attend_step(step, _):
        g, i = step // chips, lax.rem(step, chips)
        mine = jnp.logical_or(jnp.logical_and(g > 0, lax.rem(g, 2) == 0), g == last)
        k = jnp.where(g == 0, 0, jnp.where(mine, (g - 1) // 2, (g + 1) // 2))
        own_side = half * chips + lax.rem(place // CORES + 1 + i, chips)
        chip = jnp.where(mine, own_side, (1 - half) * chips + i)
        here = pl.ds(pl.multiple_of(chip * tile, tile), tile)

        @pl.when(jnp.logical_and(i == 0, jnp.logical_not(mine)))
        def _():
            drain(kv.at[k], kv_recv.at[k])
            kv[k, 0] = column_norm(kv[k, 0].astype(jnp.float32), gains[1, :, owned_chunk(s, k)])
            query_copy(k).wait_recv()

        values = kv[k, 1]
        keys = kv[k, 0]
        queries = qbuf[k, here]
        results = []
        for mask in (first, jnp.logical_not(first)):
            masked = jnp.where(mask, queries, jnp.zeros_like(queries))
            scores = lax.dot_general(
                masked, keys, (((1,), (1,)), ((), ())), preferred_element_type=jnp.float32)
            largest = jnp.max(scores, axis=-1, keepdims=True)
            probability = jnp.exp2((scores - largest) * exponent)
            normaliser = jnp.sum(probability, axis=-1, keepdims=True)
            blended = jnp.dot(
                probability.astype(jnp.bfloat16), values, preferred_element_type=jnp.float32)
            results.append(blended / normaliser)
        obuf[k, here] = jnp.where(first, results[0], results[1]).astype(jnp.bfloat16)
        for c in range(CORES):
            to = chip * CORES + c

            @pl.when(to != s)
            def _():
                out_copy(k, to).start()

            @pl.when(to == s)
            def _():
                out[:, owned_chunk(s, k)] = obuf[k, all_rows_of(s)]

        return 0

    lax.fori_loop(0, 2 * chunks * chips, attend_step, 0)

    drain(pbuf.at[pl.ds(0, (2 * chips - 1) * tokens)], p_send.at[0])
    drain(wbuf.at[:, pl.ds(0, 3 * rows)], w_send.at[0])
    drain(kv.at[:, :, pl.ds(0, (n - 1) * tokens)], kv_send.at[0])
    drain(qsend, q_send.at[0])
    drain(obuf.at[:, pl.ds(0, (n - 1) * tokens)], o_send.at[0])
    drain(out.at[:, pl.ds(0, (n - 1) * width)], o_recv.at[0])


def fused_per_device(n, fn, patches, weight_codes, block_scales, key_proj, value_proj, query_gain, key_gain):
    _, tokens, features = patches.shape
    rows, columns = weight_codes.shape
    width = columns // n
    chunks = width // LANES
    group = n // 2 * tokens
    chips = n // 2 // CORES
    bf16 = jnp.bfloat16
    dma = pltpu.SemaphoreType.DMA
    anywhere = pl.BlockSpec(memory_space=pl.ANY)
    result = pl.pallas_call(
        functools.partial(fused_kernel, n, fn),
        out_shape=pltpu.VMEM((tokens, columns), bf16),
        in_specs=[anywhere] * 7,
        out_specs=pl.BlockSpec(memory_space=pltpu.VMEM),
        scratch_shapes=[
            pltpu.VMEM((group, features), bf16),
            pltpu.VMEM((2 * chunks, rows, LANES), jnp.int32),
            pltpu.VMEM((chunks, features, 2 * LANES), bf16),
            pltpu.VMEM((chunks, 2, n * tokens, LANES), bf16),
            pltpu.VMEM((chunks, group, LANES), bf16),
            pltpu.VMEM((chunks, n * tokens, LANES), bf16),
            pltpu.VMEM((chunks, n * tokens, LANES), bf16),
            pltpu.VMEM((2, 1, columns), jnp.float32),
            pltpu.SMEM(block_scales.shape, jnp.float32),
            dma((1,)), dma((1,)), dma((1,)), dma((chips - 1,)), dma((1,)), dma((1,)),
            dma((chunks,)), dma((chunks,)), dma((1,)),
            dma((1,)), dma((chunks,)), dma((1,)), dma((chunks,)), dma((1,)), dma((1,)),
        ],
        compiler_params=pltpu.CompilerParams(
            collective_id=0, has_side_effects=True, vmem_limit_bytes=56 * 1024 * 1024),
    )(
        patches.reshape(tokens, features), weight_codes, block_scales,
        key_proj.reshape(tokens, columns), value_proj.reshape(tokens, columns),
        query_gain.reshape(1, columns), key_gain.reshape(1, columns),
    )
    return result.reshape(1, tokens, columns)


def solution(mesh):
    n, fn = mesh.shape["seq"], mesh.shape["fsdp"]
    specs = (
        P("fsdp", "seq", None), P("fsdp", None), P("fsdp", None),
        P("fsdp", "seq", None), P("fsdp", "seq", None), P(), P(),
    )

    def whole(*arrays):
        patches, weight_codes = arrays[:2]
        fits = patches.shape[0] == fn == GRID * GRID and weight_codes.shape[1] % (n * LANES) == 0 and n % (2 * CORES) == 0 and n > 2 * CORES
        body = functools.partial(fused_per_device, n, fn) if fits else per_device
        return jax.shard_map(
            body, mesh=mesh, in_specs=specs, out_specs=P("fsdp", "seq", None), check_vma=False
        )(*arrays)

    return whole
```

```python
import functools
import math
import jax
import jax.numpy as jnp
from jax import lax
from jax.experimental import pallas as pl
from jax.experimental.pallas import tpu as pltpu
from jax.sharding import PartitionSpec as P

HEADS = 48
HDIM = 64
BLOCK = 128


NORM_FLOOR = 0.25


def head_norm(projected, gain_row):
    shaped = projected.reshape(projected.shape[:-1] + (HEADS, HDIM))
    average = jnp.mean(shaped, axis=-1, keepdims=True)
    centred = shaped - average
    spread = jnp.mean(centred * centred, axis=-1, keepdims=True)
    normed = centred * lax.rsqrt(spread + NORM_FLOOR) * gain_row.reshape(HEADS, HDIM)
    return normed.astype(jnp.bfloat16)


def dequantize(weight_codes, block_scales):
    row_count, column_count = weight_codes.shape
    blocked = weight_codes.astype(jnp.float32).reshape(
        row_count // BLOCK, BLOCK, column_count // BLOCK, BLOCK
    )
    return (
        (blocked * block_scales[:, None, :, None])
        .reshape(row_count, column_count)
        .astype(jnp.bfloat16)
    )


def start_of(query_view):
    image_count, token_count, head_count = (
        query_view.shape[0],
        query_view.shape[1],
        query_view.shape[2],
    )
    return (
        jnp.full((image_count, token_count, head_count), -1e30, jnp.float32),
        jnp.zeros((image_count, token_count, head_count), jnp.float32),
        jnp.zeros(query_view.shape, jnp.float32),
    )


def attend_block(query_view, state_now, key_view, value_view):
    running_max, running_sum, weighted = state_now
    scores = jnp.einsum(
        "ithd,ishd->iths", query_view, key_view, preferred_element_type=jnp.float32
    ) * HDIM ** (-0.5)
    newest = jnp.maximum(running_max, jnp.max(scores, axis=-1))
    probability = jnp.exp(scores - newest[..., None])
    running_sum = jnp.sum(probability, axis=-1)
    blended = jnp.einsum(
        "iths,ishd->ithd",
        probability.astype(jnp.bfloat16),
        value_view,
        preferred_element_type=jnp.float32,
    )
    weighted = blended
    return (newest, running_sum, weighted)


def per_device(patches, weight_codes, block_scales, key_proj, value_proj, query_gain, key_gain):
    image_count, token_count, feature_count = patches.shape
    flat_rows = patches.reshape(image_count * token_count, feature_count)
    key_norm = head_norm(key_proj.astype(jnp.float32), key_gain)
    value_view = value_proj.reshape(image_count, token_count, HEADS, HDIM)
    local_weight = dequantize(weight_codes, block_scales)
    group_rows = lax.all_to_all(flat_rows, "fsdp", split_axis=1, concat_axis=0, tiled=True)
    queries = lax.psum_scatter(
        jnp.dot(group_rows, local_weight, preferred_element_type=jnp.float32),
        "fsdp",
        scatter_dimension=0,
        tiled=True,
    )
    query_view = head_norm(queries, query_gain).reshape(image_count, token_count, HEADS, HDIM)
    finished = attend_block(
        query_view,
        start_of(query_view),
        lax.all_gather(key_norm, "seq", axis=1, tiled=True),
        lax.all_gather(value_view, "seq", axis=1, tiled=True),
    )
    attended = finished[2] / finished[1][..., None]
    return attended.reshape(image_count, token_count, HEADS * HDIM).astype(jnp.bfloat16)


MESH = pl.DeviceIdType.MESH
LANES = 128
CORES = 2
GRID = 2


def column_norm(values, gain_row):
    lane = lambda axis: lax.broadcasted_iota(jnp.int32, (LANES, LANES), axis) < HDIM
    spread_out = jnp.where(lane(0) == lane(1), 1.0 / HDIM, 0.0).astype(jnp.bfloat16)
    spread_out = jnp.concatenate([spread_out, spread_out], axis=0)

    def mean_of(t):
        high = t.astype(jnp.bfloat16)
        low = (t - high.astype(jnp.float32)).astype(jnp.bfloat16)
        return jnp.dot(jnp.concatenate([high, low], axis=1), spread_out, preferred_element_type=jnp.float32)

    centred = values - mean_of(values)
    normed = centred * lax.rsqrt(mean_of(centred * centred) + NORM_FLOOR) * gain_row
    return normed.astype(jnp.bfloat16)


def attend_order(chunks, chips):
    order, late = [], []
    for k in range(chunks):
        order += [(0, k, i, int(i == 0)) for i in range(chips if k == 0 else 1)]
        order += late
        late = [(0, k, i, 0) for i in range(1, chips)] if k > 0 else []
        if k == chunks - 1:
            order += late
        order += [(1, k, i, 0) for i in range(chips)]
    return order


def fused_kernel(
    n, fn, patches, codes, scales_in, key, value, query_gain_in, key_gain_in, out,
    pbuf, cbuf, wbuf, own, kv, qsend, qbuf, obuf, gains, scales,
    own_sem, code_sem, scale_sem, gain_sem, mate_recv, rest_recv, p_send, near_recv, relay_recv, w_send,
    kv_send, kv_recv, q_send, q_recv, o_send, o_recv,
):
    s, f = lax.axis_index("seq"), lax.axis_index("fsdp")
    m = n // 2
    half, place = s // m, lax.rem(s, m)
    tokens = patches.shape[0]
    rows, columns = codes.shape
    width = columns // n
    chunks = width // LANES
    group = m * tokens
    chips = m // CORES
    core = lax.rem(s, CORES)
    partner = s + 1 - 2 * core

    barrier = pltpu.get_barrier_semaphore()
    for d in range(1, n):
        pl.semaphore_signal(barrier, inc=1, device_id={"seq": lax.rem(s + d, n)}, device_id_type=MESH)
    for d in range(1, fn):
        pl.semaphore_signal(barrier, inc=1, device_id={"fsdp": lax.rem(f + d, fn)}, device_id_type=MESH)

    def chip_mate(d):
        return half * m + lax.rem(place + d * CORES, m)

    def rows_of(device):
        return pl.ds(pl.multiple_of(lax.rem(device, m) * tokens, tokens), tokens)

    def all_rows_of(device):
        return pl.ds(pl.multiple_of(device * tokens, tokens), tokens)

    def owned(device):
        return pl.multiple_of((lax.rem(device, m) * 2 + device // m) * width, LANES)

    def owned_chunk(device, k):
        return pl.ds(pl.multiple_of(owned(device) + k * LANES, LANES), LANES)

    def chunk_column(q):
        side = jnp.where(q < chunks, 1 - half, half)
        return pl.multiple_of((place * 2 + side) * width + lax.rem(q, chunks) * LANES, LANES)

    def drain(ref, sem):
        pltpu.make_async_copy(ref, ref, sem).wait()

    pltpu.make_async_copy(patches, pbuf.at[rows_of(s)], own_sem.at[0]).start()
    for which, src in enumerate((key, value)):
        pltpu.make_async_copy(src, own.at[which], own_sem.at[1]).start()
    pltpu.make_async_copy(scales_in, scales, scale_sem.at[0]).start()
    for q in range(2 * chunks):
        pltpu.make_async_copy(codes.at[:, pl.ds(chunk_column(q), LANES)], cbuf.at[q], code_sem.at[0]).start()

    pl.semaphore_wait(barrier, n - 1 + fn - 1)
    drain(pbuf.at[rows_of(s)], own_sem.at[0])

    def remote(src, dst, send, recv, **device):
        return pltpu.make_async_remote_copy(
            src_ref=src, dst_ref=dst, send_sem=send, recv_sem=recv, device_id=device, device_id_type=MESH)

    def mate_copy(d):
        return remote(pbuf.at[rows_of(s)], pbuf.at[rows_of(s)], p_send.at[0], mate_recv.at[d - 1], seq=chip_mate(d))

    for d in range(1, chips):
        mate_copy(d).start()

    far = place // CORES == jnp.where(half == 0, 0, chips - 1)

    def start_kv(to):
        def one(k, _):
            for which in range(2):
                remote(
                    own.at[which, :, owned_chunk(to, k)], kv.at[k, which, all_rows_of(s)],
                    kv_send.at[0], kv_recv.at[k], seq=to).start()
            return 0

        return one

    def start_chip(chip, low, high):
        def both(k, _):
            for c in range(CORES):
                start_kv(chip * CORES + c)(k, 0)
            return 0

        lax.fori_loop(low, high, both, 0)

    def across(j):
        return jnp.where(half == 0, chips + j, chips - 1 - j)

    def beside(low, high):
        for d in range(1, chips):
            start_chip(chip_mate(d) // CORES, low, high)

    drain(own, own_sem.at[1])
    start_chip(across(0), 0, chunks)
    pltpu.make_async_copy(query_gain_in, gains.at[0], gain_sem.at[0]).start()
    pltpu.make_async_copy(key_gain_in, gains.at[1], gain_sem.at[0]).start()
    for k in range(chunks):
        for which, src in enumerate((key, value)):
            pltpu.make_async_copy(
                src.at[:, owned_chunk(s, k)], kv.at[k, which, all_rows_of(s)], kv_recv.at[k]).start()
    pl.when(far)(lambda: beside(0, 1))
    for j in range(1, chips):
        start_chip(across(j), 0, chunks)
    remote(pbuf.at[rows_of(s)], pbuf.at[rows_of(s)], p_send.at[0], rest_recv.at[0], seq=partner).start()
    lax.fori_loop(0, chunks, start_kv(partner), 0)

    row_mate = f + 1 - 2 * lax.rem(f, GRID)
    column_mate = lax.rem(f + GRID, fn)

    def weight_copy(pair, recv, start, size, to):
        at = pl.ds(pl.multiple_of(start, size), size)
        return remote(wbuf.at[pair, at], wbuf.at[pair, at], w_send.at[0], recv.at[pair], fsdp=to)

    part = rows // 2

    def near_start(pair, start, size):
        for mate in (row_mate, column_mate):
            weight_copy(pair, near_recv, f * rows + start, size, mate).start()

    def relay(pair):
        drain(wbuf.at[pair, pl.ds(0, 2 * rows)], near_recv.at[pair])
        weight_copy(pair, relay_recv, row_mate * rows, part, column_mate).start()
        weight_copy(pair, relay_recv, column_mate * rows + part, part, row_mate).start()

    drain(scales, scale_sem.at[0])
    drain(cbuf, code_sem.at[0])

    def dequantize_pair(pair, _):
        for side in range(2):
            q = 2 * pair + side
            for block in range(rows // BLOCK):
                scale = scales[block, chunk_column(q) // BLOCK]
                piece = cbuf[q, block * BLOCK:(block + 1) * BLOCK, :].astype(jnp.float32) * scale
                at = pl.ds(pl.multiple_of(f * rows + block * BLOCK, BLOCK), BLOCK)
                wbuf[pair, at, side * LANES:(side + 1) * LANES] = piece.astype(jnp.bfloat16)

        @pl.when(pair == 0)
        def _():
            near_start(pair, 0, rows)

        @pl.when(pair == 1)
        def _():
            near_start(pair, 0, part)

        return 0

    lax.fori_loop(0, chunks, dequantize_pair, 0)

    def patches_in():
        for d in range(1, chips):
            at = rows_of(half * m + lax.rem(place + m - d * CORES, m))
            drain(pbuf.at[at], mate_recv.at[d - 1])
            remote(pbuf.at[at], pbuf.at[at], p_send.at[0], rest_recv.at[0], seq=partner).start()
        drain(pbuf.at[pl.ds(0, chips * tokens)], rest_recv.at[0])

    def relay_rest():
        for pair in range(1, chunks - 1):
            relay(pair)
            near_start(pair + 1, 0, rows)

    relay(0)
    near_start(1, part, part)
    pl.when(far)(relay_rest)
    patches_in()
    drain(gains, gain_sem.at[0])

    other = lax.rem(s + m, n)
    half_rows = pl.ds(pl.multiple_of(half * group, group), group)

    def query_copy(k):
        return remote(qsend.at[k], qbuf.at[k, half_rows], q_send.at[0], q_recv.at[k], seq=other)

    def project(pair):
        drain(wbuf.at[pair, pl.ds(0, rows)], relay_recv.at[pair])
        both = jnp.dot(pbuf[...], wbuf[pair], preferred_element_type=jnp.float32)
        for side in range(2):
            q = 2 * pair + side
            normed = column_norm(
                both[:, side * LANES:(side + 1) * LANES], gains[0, :, pl.ds(chunk_column(q), LANES)])
            if q < chunks:
                qsend[q] = normed
                query_copy(q).start()
            else:
                qbuf[q - chunks, half_rows] = normed

    project(0)
    pl.when(jnp.logical_not(far))(relay_rest)
    for pair in range(1, chunks - 1):
        project(pair)
    beside(jnp.where(far, 1, 0), chunks)
    relay(chunks - 1)
    project(chunks - 1)

    tile = CORES * tokens
    exponent = HDIM ** (-0.5) * math.log2(math.e)

    def out_copy(k, to):
        return remote(obuf.at[k, all_rows_of(to)], out.at[:, owned_chunk(s, k)], o_send.at[0], o_recv.at[0], seq=to)

    first = lax.broadcasted_iota(jnp.int32, (tile, LANES), 1) < HDIM

    order = attend_order(chunks, chips)

    def entry(step, column):
        return sum(jnp.where(step == at, row[column], 0) for at, row in enumerate(order))

    def attend_step(step, _):
        mine, k, i, opens = (entry(step, column) for column in range(4))
        own_side = half * chips + lax.rem(place // CORES + 1 + i, chips)
        chip = jnp.where(mine == 1, own_side, across(chips - 1 - i))
        here = pl.ds(pl.multiple_of(chip * tile, tile), tile)

        @pl.when(opens == 1)
        def _():
            drain(kv.at[k], kv_recv.at[k])
            kv[k, 0] = column_norm(kv[k, 0].astype(jnp.float32), gains[1, :, owned_chunk(s, k)])
            query_copy(k).wait_recv()

        values = kv[k, 1]
        keys = kv[k, 0]
        queries = qbuf[k, here]
        results = []
        for mask in (first, jnp.logical_not(first)):
            masked = jnp.where(mask, queries, jnp.zeros_like(queries))
            scores = lax.dot_general(
                masked, keys, (((1,), (1,)), ((), ())), preferred_element_type=jnp.float32)
            largest = jnp.max(scores, axis=-1, keepdims=True)
            probability = jnp.exp2((scores - largest) * exponent)
            normaliser = jnp.sum(probability, axis=-1, keepdims=True)
            blended = jnp.dot(
                probability.astype(jnp.bfloat16), values, preferred_element_type=jnp.float32)
            results.append(blended / normaliser)
        obuf[k, here] = jnp.where(first, results[0], results[1]).astype(jnp.bfloat16)
        for c in range(CORES):
            to = chip * CORES + c

            @pl.when(to != s)
            def _():
                out_copy(k, to).start()

            @pl.when(to == s)
            def _():
                out[:, owned_chunk(s, k)] = obuf[k, all_rows_of(s)]

        return 0

    lax.fori_loop(0, len(order), attend_step, 0)

    drain(pbuf.at[pl.ds(0, (2 * chips - 1) * tokens)], p_send.at[0])
    drain(wbuf.at[:, pl.ds(0, 3 * rows)], w_send.at[0])
    drain(kv.at[:, :, pl.ds(0, (n - 1) * tokens)], kv_send.at[0])
    drain(qsend, q_send.at[0])
    drain(obuf.at[:, pl.ds(0, (n - 1) * tokens)], o_send.at[0])
    drain(out.at[:, pl.ds(0, (n - 1) * width)], o_recv.at[0])


def fused_per_device(n, fn, patches, weight_codes, block_scales, key_proj, value_proj, query_gain, key_gain):
    _, tokens, features = patches.shape
    rows, columns = weight_codes.shape
    width = columns // n
    chunks = width // LANES
    group = n // 2 * tokens
    chips = n // 2 // CORES
    bf16 = jnp.bfloat16
    dma = pltpu.SemaphoreType.DMA
    anywhere = pl.BlockSpec(memory_space=pl.ANY)
    result = pl.pallas_call(
        functools.partial(fused_kernel, n, fn),
        out_shape=pltpu.VMEM((tokens, columns), bf16),
        in_specs=[anywhere] * 7,
        out_specs=pl.BlockSpec(memory_space=pltpu.VMEM),
        scratch_shapes=[
            pltpu.VMEM((group, features), bf16),
            pltpu.VMEM((2 * chunks, rows, LANES), jnp.int32),
            pltpu.VMEM((chunks, features, 2 * LANES), bf16),
            pltpu.VMEM((2, tokens, columns), bf16),
            pltpu.VMEM((chunks, 2, n * tokens, LANES), bf16),
            pltpu.VMEM((chunks, group, LANES), bf16),
            pltpu.VMEM((chunks, n * tokens, LANES), bf16),
            pltpu.VMEM((chunks, n * tokens, LANES), bf16),
            pltpu.VMEM((2, 1, columns), jnp.float32),
            pltpu.SMEM(block_scales.shape, jnp.float32),
            dma((2,)), dma((1,)), dma((1,)), dma((1,)), dma((chips - 1,)), dma((1,)), dma((1,)),
            dma((chunks,)), dma((chunks,)), dma((1,)),
            dma((1,)), dma((chunks,)), dma((1,)), dma((chunks,)), dma((1,)), dma((1,)),
        ],
        compiler_params=pltpu.CompilerParams(
            collective_id=0, has_side_effects=True, vmem_limit_bytes=56 * 1024 * 1024),
    )(
        patches.reshape(tokens, features), weight_codes, block_scales,
        key_proj.reshape(tokens, columns), value_proj.reshape(tokens, columns),
        query_gain.reshape(1, columns), key_gain.reshape(1, columns),
    )
    return result.reshape(1, tokens, columns)


def solution(mesh):
    n, fn = mesh.shape["seq"], mesh.shape["fsdp"]
    specs = (
        P("fsdp", "seq", None), P("fsdp", None), P("fsdp", None),
        P("fsdp", "seq", None), P("fsdp", "seq", None), P(), P(),
    )

    def whole(*arrays):
        patches, weight_codes = arrays[:2]
        fits = patches.shape[0] == fn == GRID * GRID and weight_codes.shape[1] % (n * LANES) == 0 and n % (2 * CORES) == 0 and n > 2 * CORES
        body = functools.partial(fused_per_device, n, fn) if fits else per_device
        return jax.shard_map(
            body, mesh=mesh, in_specs=specs, out_specs=P("fsdp", "seq", None), check_vma=False
        )(*arrays)

    return whole
```

```python
import functools
import math
import jax
import jax.numpy as jnp
from jax import lax
from jax.experimental import pallas as pl
from jax.experimental.pallas import tpu as pltpu
from jax.sharding import PartitionSpec as P

HEADS = 48
HDIM = 64
BLOCK = 128


NORM_FLOOR = 0.25


def head_norm(projected, gain_row):
    shaped = projected.reshape(projected.shape[:-1] + (HEADS, HDIM))
    average = jnp.mean(shaped, axis=-1, keepdims=True)
    centred = shaped - average
    spread = jnp.mean(centred * centred, axis=-1, keepdims=True)
    normed = centred * lax.rsqrt(spread + NORM_FLOOR) * gain_row.reshape(HEADS, HDIM)
    return normed.astype(jnp.bfloat16)


def dequantize(weight_codes, block_scales):
    row_count, column_count = weight_codes.shape
    blocked = weight_codes.astype(jnp.float32).reshape(
        row_count // BLOCK, BLOCK, column_count // BLOCK, BLOCK
    )
    return (
        (blocked * block_scales[:, None, :, None])
        .reshape(row_count, column_count)
        .astype(jnp.bfloat16)
    )


def start_of(query_view):
    image_count, token_count, head_count = (
        query_view.shape[0],
        query_view.shape[1],
        query_view.shape[2],
    )
    return (
        jnp.full((image_count, token_count, head_count), -1e30, jnp.float32),
        jnp.zeros((image_count, token_count, head_count), jnp.float32),
        jnp.zeros(query_view.shape, jnp.float32),
    )


def attend_block(query_view, state_now, key_view, value_view):
    running_max, running_sum, weighted = state_now
    scores = jnp.einsum(
        "ithd,ishd->iths", query_view, key_view, preferred_element_type=jnp.float32
    ) * HDIM ** (-0.5)
    newest = jnp.maximum(running_max, jnp.max(scores, axis=-1))
    probability = jnp.exp(scores - newest[..., None])
    running_sum = jnp.sum(probability, axis=-1)
    blended = jnp.einsum(
        "iths,ishd->ithd",
        probability.astype(jnp.bfloat16),
        value_view,
        preferred_element_type=jnp.float32,
    )
    weighted = blended
    return (newest, running_sum, weighted)


def per_device(patches, weight_codes, block_scales, key_proj, value_proj, query_gain, key_gain):
    image_count, token_count, feature_count = patches.shape
    flat_rows = patches.reshape(image_count * token_count, feature_count)
    key_norm = head_norm(key_proj.astype(jnp.float32), key_gain)
    value_view = value_proj.reshape(image_count, token_count, HEADS, HDIM)
    local_weight = dequantize(weight_codes, block_scales)
    group_rows = lax.all_to_all(flat_rows, "fsdp", split_axis=1, concat_axis=0, tiled=True)
    queries = lax.psum_scatter(
        jnp.dot(group_rows, local_weight, preferred_element_type=jnp.float32),
        "fsdp",
        scatter_dimension=0,
        tiled=True,
    )
    query_view = head_norm(queries, query_gain).reshape(image_count, token_count, HEADS, HDIM)
    finished = attend_block(
        query_view,
        start_of(query_view),
        lax.all_gather(key_norm, "seq", axis=1, tiled=True),
        lax.all_gather(value_view, "seq", axis=1, tiled=True),
    )
    attended = finished[2] / finished[1][..., None]
    return attended.reshape(image_count, token_count, HEADS * HDIM).astype(jnp.bfloat16)


MESH = pl.DeviceIdType.MESH
LANES = 128
CORES = 2
GRID = 2


def column_norm(values, gain_row):
    lane = lambda axis: lax.broadcasted_iota(jnp.int32, (LANES, LANES), axis) < HDIM
    spread_out = jnp.where(lane(0) == lane(1), 1.0 / HDIM, 0.0).astype(jnp.bfloat16)
    spread_out = jnp.concatenate([spread_out, spread_out], axis=0)

    def mean_of(t):
        high = t.astype(jnp.bfloat16)
        low = (t - high.astype(jnp.float32)).astype(jnp.bfloat16)
        return jnp.dot(jnp.concatenate([high, low], axis=1), spread_out, preferred_element_type=jnp.float32)

    centred = values - mean_of(values)
    normed = centred * lax.rsqrt(mean_of(centred * centred) + NORM_FLOOR) * gain_row
    return normed.astype(jnp.bfloat16)


def attend_order(chunks, chips):
    order, late = [], []
    for k in range(chunks):
        order += [(0, k, i, int(i == 0)) for i in range(chips if k == 0 else 1)]
        order += late
        late = [(0, k, i, 0) for i in range(1, chips)] if k > 0 else []
        if k == chunks - 1:
            order += late
        order += [(1, k, i, 0) for i in range(chips)]
    return order


def fused_kernel(
    n, fn, patches, codes, scales_in, key, value, query_gain_in, key_gain_in, out,
    pbuf, cbuf, wbuf, own, kv, qsend, qbuf, obuf, gains, scales,
    own_sem, code_sem, scale_sem, gain_sem, mate_recv, rest_recv, p_send, first_recv, rest_w_recv, w_send,
    kv_send, kv_recv, q_send, q_recv, o_send, o_recv, met,
):
    s, f = lax.axis_index("seq"), lax.axis_index("fsdp")
    m = n // 2
    half, place = s // m, lax.rem(s, m)
    tokens = patches.shape[0]
    rows, columns = codes.shape
    width = columns // n
    chunks = width // LANES
    group = m * tokens
    chips = m // CORES
    core = lax.rem(s, CORES)
    partner = s + 1 - 2 * core

    barrier = pltpu.get_barrier_semaphore()
    far = place // CORES == jnp.where(half == 0, 0, chips - 1)
    near = jnp.logical_not(far)
    row_mate = f + 1 - 2 * lax.rem(f, GRID)
    column_mate = lax.rem(f + GRID, fn)

    beside_device = half * m + lax.rem(place + CORES, m)
    def across(j):
        return jnp.where(half == 0, chips + j, chips - 1 - j)

    def greet(semaphore, chip):
        for c in range(CORES):
            pl.semaphore_signal(semaphore, inc=1, device_id={"seq": chip * CORES + c}, device_id_type=MESH)

    beside_chip = beside_device // CORES

    @pl.when(near)
    def _():
        greet(barrier, across(0))
        greet(barrier, beside_chip)

    @pl.when(jnp.logical_and(far, half == 1))
    def _():
        greet(barrier, beside_chip)

    pl.semaphore_signal(barrier, inc=1, device_id={"seq": partner}, device_id_type=MESH)
    for mate in (row_mate, column_mate):
        pl.semaphore_signal(barrier, inc=1, device_id={"fsdp": mate}, device_id_type=MESH)

    def rows_of(device):
        return pl.ds(pl.multiple_of(lax.rem(device, m) * tokens, tokens), tokens)

    def all_rows_of(device):
        return pl.ds(pl.multiple_of(device * tokens, tokens), tokens)

    def owned(device):
        return pl.multiple_of((lax.rem(device, m) * 2 + device // m) * width, LANES)

    def owned_chunk(device, k):
        return pl.ds(pl.multiple_of(owned(device) + k * LANES, LANES), LANES)

    def chunk_column(q):
        side = jnp.where(q < chunks, 1 - half, half)
        return pl.multiple_of((place * 2 + side) * width + lax.rem(q, chunks) * LANES, LANES)

    def drain(ref, sem):
        pltpu.make_async_copy(ref, ref, sem).wait()

    pltpu.make_async_copy(patches, pbuf.at[rows_of(s)], own_sem.at[0]).start()
    for which, src in enumerate((key, value)):
        pltpu.make_async_copy(src, own.at[which], own_sem.at[1]).start()
    pltpu.make_async_copy(scales_in, scales, scale_sem.at[0]).start()
    for q in range(2 * chunks):
        pltpu.make_async_copy(codes.at[:, pl.ds(chunk_column(q), LANES)], cbuf.at[q], code_sem.at[0]).start()

    pl.semaphore_wait(barrier, CORES + 3 + jnp.where(jnp.logical_and(near, half == 1), CORES, 0))

    def remote(src, dst, send, recv, **device):
        return pltpu.make_async_remote_copy(
            src_ref=src, dst_ref=dst, send_sem=send, recv_sem=recv, device_id=device, device_id_type=MESH)

    def mate_copy():
        return remote(pbuf.at[rows_of(s)], pbuf.at[rows_of(s)], p_send.at[0], mate_recv.at[0], seq=beside_device)

    def start_kv(to):
        def one(unit, _):
            k, which = unit // 2, lax.rem(unit, 2)
            remote(
                own.at[which, :, owned_chunk(to, k)], kv.at[k, which, all_rows_of(s)],
                kv_send.at[0], kv_recv.at[k], seq=to).start()
            return 0

        return one

    def start_chip(chip, low, high):
        def both(unit, _):
            for c in range(CORES):
                start_kv(chip * CORES + c)(unit, 0)
            return 0

        lax.fori_loop(low, high, both, 0)

    early_units = jnp.where(half == 0, 3, 2)

    def beside(low, high):
        start_chip(beside_chip, low, high)

    @pl.when(near)
    def _():
        drain(own, own_sem.at[1])
        start_chip(across(0), 0, 2 * chunks)

        @pl.when(half == 0)
        def _():
            pl.semaphore_wait(met.at[1], CORES)

        greet(met.at[0], beside_chip)
        greet(met.at[2], across(0))
        drain(pbuf.at[rows_of(s)], own_sem.at[0])
        mate_copy().start()

    @pl.when(far)
    def _():
        pl.when(half == 0)(lambda: greet(met.at[1], beside_chip))
        drain(pbuf.at[rows_of(s)], own_sem.at[0])
        mate_copy().start()

    for k in range(chunks):
        for which, src in enumerate((key, value)):
            pltpu.make_async_copy(
                src.at[:, owned_chunk(s, k)], kv.at[k, which, all_rows_of(s)], kv_recv.at[k]).start()
    pltpu.make_async_copy(query_gain_in, gains.at[0], gain_sem.at[0]).start()
    pltpu.make_async_copy(key_gain_in, gains.at[1], gain_sem.at[0]).start()

    def weight_copy(pair, recv, start, size, to):
        at = pl.ds(pl.multiple_of(start, size), size)
        return remote(wbuf.at[pair, at], wbuf.at[pair, at], w_send.at[0], recv.at[pair], fsdp=to)

    part = rows // 2

    def weights_out(pair):
        for recv, row_half in ((first_recv, 0), (rest_w_recv, part)):
            weight_copy(pair, recv, f * rows + row_half, part, row_mate).start()
            weight_copy(pair, recv, f * rows + part - row_half, part, column_mate).start()

    def relay(pair):
        drain(wbuf.at[pair, pl.ds(0, rows)], first_recv.at[pair])
        weight_copy(pair, rest_w_recv, row_mate * rows, part, column_mate).start()
        weight_copy(pair, rest_w_recv, column_mate * rows + part, part, row_mate).start()

    drain(scales, scale_sem.at[0])
    drain(cbuf, code_sem.at[0])

    def dequantize_pair(pair, _):
        for side in range(2):
            q = 2 * pair + side
            for block in range(rows // BLOCK):
                scale = scales[block, chunk_column(q) // BLOCK]
                piece = cbuf[q, block * BLOCK:(block + 1) * BLOCK, :].astype(jnp.float32) * scale
                at = pl.ds(pl.multiple_of(f * rows + block * BLOCK, BLOCK), BLOCK)
                wbuf[pair, at, side * LANES:(side + 1) * LANES] = piece.astype(jnp.bfloat16)

        pl.when(pair == 0)(lambda: weights_out(0))
        return 0

    lax.fori_loop(0, chunks, dequantize_pair, 0)

    @pl.when(near)
    def _():
        pl.semaphore_wait(met.at[2], CORES)
        greet(met.at[3], beside_chip)

    @pl.when(far)
    def _():
        drain(own, own_sem.at[1])
        pl.semaphore_wait(met.at[0], CORES)
        start_chip(across(0), 0, 2 * chunks)
        beside(0, early_units)
        pl.semaphore_wait(met.at[3], CORES)

    start_chip(across(1), 0, 2 * chunks)
    remote(pbuf.at[rows_of(s)], pbuf.at[rows_of(s)], p_send.at[0], rest_recv.at[0], seq=partner).start()
    lax.fori_loop(0, 2 * chunks, start_kv(partner), 0)

    def forward():
        at = rows_of(beside_device)
        drain(pbuf.at[at], mate_recv.at[0])
        remote(pbuf.at[at], pbuf.at[at], p_send.at[0], rest_recv.at[0], seq=partner).start()

    relay(0)
    weights_out(1)
    pl.when(near)(forward)
    for pair in range(1, chunks - 1):
        relay(pair)
        weights_out(pair + 1)
    pl.when(far)(forward)
    drain(gains, gain_sem.at[0])
    drain(pbuf.at[pl.ds(0, chips * tokens)], rest_recv.at[0])

    other = lax.rem(s + m, n)
    half_rows = pl.ds(pl.multiple_of(half * group, group), group)

    def query_copy(k):
        return remote(qsend.at[k], qbuf.at[k, half_rows], q_send.at[0], q_recv.at[k], seq=other)

    def project(pair):
        drain(wbuf.at[pair, pl.ds(0, 2 * rows)], rest_w_recv.at[pair])
        both = jnp.dot(pbuf[...], wbuf[pair], preferred_element_type=jnp.float32)
        for side in range(2):
            q = 2 * pair + side
            normed = column_norm(
                both[:, side * LANES:(side + 1) * LANES], gains[0, :, pl.ds(chunk_column(q), LANES)])
            if q < chunks:
                qsend[q] = normed
                query_copy(q).start()
            else:
                qbuf[q - chunks, half_rows] = normed

    for pair in range(chunks - 1):
        project(pair)
    beside(jnp.where(far, early_units, 0), 2 * chunks)
    relay(chunks - 1)
    project(chunks - 1)

    tile = CORES * tokens
    exponent = HDIM ** (-0.5) * math.log2(math.e)

    def out_copy(k, to):
        return remote(obuf.at[k, all_rows_of(to)], out.at[:, owned_chunk(s, k)], o_send.at[0], o_recv.at[0], seq=to)

    first = lax.broadcasted_iota(jnp.int32, (tile, LANES), 1) < HDIM

    order = attend_order(chunks, chips)

    def entry(step, column):
        return sum(jnp.where(step == at, row[column], 0) for at, row in enumerate(order))

    def attend_step(step, _):
        mine, k, i, opens = (entry(step, column) for column in range(4))
        own_side = half * chips + lax.rem(place // CORES + 1 + i, chips)
        chip = jnp.where(mine == 1, own_side, across(chips - 1 - i))
        here = pl.ds(pl.multiple_of(chip * tile, tile), tile)

        @pl.when(opens == 1)
        def _():
            drain(kv.at[k], kv_recv.at[k])
            kv[k, 0] = column_norm(kv[k, 0].astype(jnp.float32), gains[1, :, owned_chunk(s, k)])
            query_copy(k).wait_recv()

        values = kv[k, 1]
        keys = kv[k, 0]
        queries = qbuf[k, here]
        results = []
        for mask in (first, jnp.logical_not(first)):
            masked = jnp.where(mask, queries, jnp.zeros_like(queries))
            scores = lax.dot_general(
                masked, keys, (((1,), (1,)), ((), ())), preferred_element_type=jnp.float32)
            largest = jnp.max(scores, axis=-1, keepdims=True)
            probability = jnp.exp2((scores - largest) * exponent)
            normaliser = jnp.sum(probability, axis=-1, keepdims=True)
            blended = jnp.dot(
                probability.astype(jnp.bfloat16), values, preferred_element_type=jnp.float32)
            results.append(blended / normaliser)
        obuf[k, here] = jnp.where(first, results[0], results[1]).astype(jnp.bfloat16)
        for c in range(CORES):
            to = chip * CORES + c

            @pl.when(to != s)
            def _():
                out_copy(k, to).start()

            @pl.when(to == s)
            def _():
                out[:, owned_chunk(s, k)] = obuf[k, all_rows_of(s)]

        return 0

    lax.fori_loop(0, len(order), attend_step, 0)

    drain(pbuf.at[pl.ds(0, (2 * chips - 1) * tokens)], p_send.at[0])
    drain(wbuf.at[:, pl.ds(0, 3 * rows)], w_send.at[0])
    drain(kv.at[:, :, pl.ds(0, (n - 1) * tokens)], kv_send.at[0])
    drain(qsend, q_send.at[0])
    drain(obuf.at[:, pl.ds(0, (n - 1) * tokens)], o_send.at[0])
    drain(out.at[:, pl.ds(0, (n - 1) * width)], o_recv.at[0])


def fused_per_device(n, fn, patches, weight_codes, block_scales, key_proj, value_proj, query_gain, key_gain):
    _, tokens, features = patches.shape
    rows, columns = weight_codes.shape
    width = columns // n
    chunks = width // LANES
    group = n // 2 * tokens
    chips = n // 2 // CORES
    bf16 = jnp.bfloat16
    dma = pltpu.SemaphoreType.DMA
    anywhere = pl.BlockSpec(memory_space=pl.ANY)
    result = pl.pallas_call(
        functools.partial(fused_kernel, n, fn),
        out_shape=pltpu.VMEM((tokens, columns), bf16),
        in_specs=[anywhere] * 7,
        out_specs=pl.BlockSpec(memory_space=pltpu.VMEM),
        scratch_shapes=[
            pltpu.VMEM((group, features), bf16),
            pltpu.VMEM((2 * chunks, rows, LANES), jnp.int32),
            pltpu.VMEM((chunks, features, 2 * LANES), bf16),
            pltpu.VMEM((2, tokens, columns), bf16),
            pltpu.VMEM((chunks, 2, n * tokens, LANES), bf16),
            pltpu.VMEM((chunks, group, LANES), bf16),
            pltpu.VMEM((chunks, n * tokens, LANES), bf16),
            pltpu.VMEM((chunks, n * tokens, LANES), bf16),
            pltpu.VMEM((2, 1, columns), jnp.float32),
            pltpu.SMEM(block_scales.shape, jnp.float32),
            dma((2,)), dma((1,)), dma((1,)), dma((1,)), dma((1,)), dma((1,)), dma((1,)),
            dma((chunks,)), dma((chunks,)), dma((1,)),
            dma((1,)), dma((chunks,)), dma((1,)), dma((chunks,)), dma((1,)), dma((1,)),
            pltpu.SemaphoreType.REGULAR((4,)),
        ],
        compiler_params=pltpu.CompilerParams(
            collective_id=0, has_side_effects=True, vmem_limit_bytes=56 * 1024 * 1024),
    )(
        patches.reshape(tokens, features), weight_codes, block_scales,
        key_proj.reshape(tokens, columns), value_proj.reshape(tokens, columns),
        query_gain.reshape(1, columns), key_gain.reshape(1, columns),
    )
    return result.reshape(1, tokens, columns)


def solution(mesh):
    n, fn = mesh.shape["seq"], mesh.shape["fsdp"]
    specs = (
        P("fsdp", "seq", None), P("fsdp", None), P("fsdp", None),
        P("fsdp", "seq", None), P("fsdp", "seq", None), P(), P(),
    )

    def whole(*arrays):
        patches, weight_codes = arrays[:2]
        fits = patches.shape[0] == fn == GRID * GRID and weight_codes.shape[1] % (n * LANES) == 0 and n == 2 * GRID * CORES
        body = functools.partial(fused_per_device, n, fn) if fits else per_device
        return jax.shard_map(
            body, mesh=mesh, in_specs=specs, out_specs=P("fsdp", "seq", None), check_vma=False
        )(*arrays)

    return whole
```

```python
import functools
import math
import jax
import jax.numpy as jnp
from jax import lax
from jax.experimental import pallas as pl
from jax.experimental.pallas import tpu as pltpu
from jax.sharding import PartitionSpec as P

HEADS = 48
HDIM = 64
BLOCK = 128


NORM_FLOOR = 0.25


def head_norm(projected, gain_row):
    shaped = projected.reshape(projected.shape[:-1] + (HEADS, HDIM))
    average = jnp.mean(shaped, axis=-1, keepdims=True)
    centred = shaped - average
    spread = jnp.mean(centred * centred, axis=-1, keepdims=True)
    normed = centred * lax.rsqrt(spread + NORM_FLOOR) * gain_row.reshape(HEADS, HDIM)
    return normed.astype(jnp.bfloat16)


def dequantize(weight_codes, block_scales):
    row_count, column_count = weight_codes.shape
    blocked = weight_codes.astype(jnp.float32).reshape(
        row_count // BLOCK, BLOCK, column_count // BLOCK, BLOCK
    )
    return (
        (blocked * block_scales[:, None, :, None])
        .reshape(row_count, column_count)
        .astype(jnp.bfloat16)
    )


def start_of(query_view):
    image_count, token_count, head_count = (
        query_view.shape[0],
        query_view.shape[1],
        query_view.shape[2],
    )
    return (
        jnp.full((image_count, token_count, head_count), -1e30, jnp.float32),
        jnp.zeros((image_count, token_count, head_count), jnp.float32),
        jnp.zeros(query_view.shape, jnp.float32),
    )


def attend_block(query_view, state_now, key_view, value_view):
    running_max, running_sum, weighted = state_now
    scores = jnp.einsum(
        "ithd,ishd->iths", query_view, key_view, preferred_element_type=jnp.float32
    ) * HDIM ** (-0.5)
    newest = jnp.maximum(running_max, jnp.max(scores, axis=-1))
    probability = jnp.exp(scores - newest[..., None])
    running_sum = jnp.sum(probability, axis=-1)
    blended = jnp.einsum(
        "iths,ishd->ithd",
        probability.astype(jnp.bfloat16),
        value_view,
        preferred_element_type=jnp.float32,
    )
    weighted = blended
    return (newest, running_sum, weighted)


def per_device(patches, weight_codes, block_scales, key_proj, value_proj, query_gain, key_gain):
    image_count, token_count, feature_count = patches.shape
    flat_rows = patches.reshape(image_count * token_count, feature_count)
    key_norm = head_norm(key_proj.astype(jnp.float32), key_gain)
    value_view = value_proj.reshape(image_count, token_count, HEADS, HDIM)
    local_weight = dequantize(weight_codes, block_scales)
    group_rows = lax.all_to_all(flat_rows, "fsdp", split_axis=1, concat_axis=0, tiled=True)
    queries = lax.psum_scatter(
        jnp.dot(group_rows, local_weight, preferred_element_type=jnp.float32),
        "fsdp",
        scatter_dimension=0,
        tiled=True,
    )
    query_view = head_norm(queries, query_gain).reshape(image_count, token_count, HEADS, HDIM)
    finished = attend_block(
        query_view,
        start_of(query_view),
        lax.all_gather(key_norm, "seq", axis=1, tiled=True),
        lax.all_gather(value_view, "seq", axis=1, tiled=True),
    )
    attended = finished[2] / finished[1][..., None]
    return attended.reshape(image_count, token_count, HEADS * HDIM).astype(jnp.bfloat16)


MESH = pl.DeviceIdType.MESH
LANES = 128
CORES = 2
GRID = 2


def column_norm(values, gain_row):
    lane = lambda axis: lax.broadcasted_iota(jnp.int32, (LANES, LANES), axis) < HDIM
    spread_out = jnp.where(lane(0) == lane(1), 1.0 / HDIM, 0.0).astype(jnp.bfloat16)
    spread_out = jnp.concatenate([spread_out, spread_out], axis=0)

    def mean_of(t):
        high = t.astype(jnp.bfloat16)
        low = (t - high.astype(jnp.float32)).astype(jnp.bfloat16)
        return jnp.dot(jnp.concatenate([high, low], axis=1), spread_out, preferred_element_type=jnp.float32)

    centred = values - mean_of(values)
    normed = centred * lax.rsqrt(mean_of(centred * centred) + NORM_FLOOR) * gain_row
    return normed.astype(jnp.bfloat16)


def attend_order(chunks, chips):
    order, late = [], []
    for k in range(chunks):
        order += [(0, k, i, int(i == 0)) for i in range(chips if k == 0 else 1)]
        order += late
        late = [(0, k, i, 0) for i in range(1, chips)] if k > 0 else []
        if k == chunks - 1:
            order += late
        order += [(1, k, i, 0) for i in range(chips)]
    return order


def fused_kernel(
    n, fn, patches, codes, scales_in, key, value, query_gain_in, key_gain_in, out,
    pbuf, cbuf, wbuf, own, kv, qsend, qbuf, obuf, gains, scales,
    own_sem, code_sem, scale_sem, gain_sem, mate_recv, partner_recv, rest_recv, p_send, first_recv, rest_w_recv, w_send,
    kv_send, kv_recv, q_send, q_recv, o_send, o_recv, met,
):
    s, f = lax.axis_index("seq"), lax.axis_index("fsdp")
    m = n // 2
    half, place = s // m, lax.rem(s, m)
    tokens = patches.shape[0]
    rows, columns = codes.shape
    width = columns // n
    chunks = width // LANES
    group = m * tokens
    chips = m // CORES
    core = lax.rem(s, CORES)
    partner = s + 1 - 2 * core

    barrier = pltpu.get_barrier_semaphore()
    far = place // CORES == jnp.where(half == 0, 0, chips - 1)
    near = jnp.logical_not(far)
    row_mate = f + 1 - 2 * lax.rem(f, GRID)
    column_mate = lax.rem(f + GRID, fn)

    beside_device = half * m + lax.rem(place + CORES, m)
    def across(j):
        return jnp.where(half == 0, chips + j, chips - 1 - j)

    def greet(semaphore, chip):
        for c in range(CORES):
            pl.semaphore_signal(semaphore, inc=1, device_id={"seq": chip * CORES + c}, device_id_type=MESH)

    beside_chip = beside_device // CORES

    @pl.when(near)
    def _():
        greet(barrier, across(0))
        greet(barrier, beside_chip)

    @pl.when(jnp.logical_and(far, half == 1))
    def _():
        greet(barrier, beside_chip)

    pl.semaphore_signal(barrier, inc=1, device_id={"seq": partner}, device_id_type=MESH)
    for mate in (row_mate, column_mate):
        pl.semaphore_signal(barrier, inc=1, device_id={"fsdp": mate}, device_id_type=MESH)

    def rows_of(device):
        return pl.ds(pl.multiple_of(lax.rem(device, m) * tokens, tokens), tokens)

    def all_rows_of(device):
        return pl.ds(pl.multiple_of(device * tokens, tokens), tokens)

    def owned(device):
        return pl.multiple_of((lax.rem(device, m) * 2 + device // m) * width, LANES)

    def owned_chunk(device, k):
        return pl.ds(pl.multiple_of(owned(device) + k * LANES, LANES), LANES)

    def chunk_column(q):
        side = jnp.where(q < chunks, 1 - half, half)
        return pl.multiple_of((place * 2 + side) * width + lax.rem(q, chunks) * LANES, LANES)

    def drain(ref, sem):
        pltpu.make_async_copy(ref, ref, sem).wait()

    pltpu.make_async_copy(patches, pbuf.at[rows_of(s)], own_sem.at[0]).start()
    for which, src in enumerate((key, value)):
        pltpu.make_async_copy(src, own.at[which], own_sem.at[1]).start()
    pltpu.make_async_copy(scales_in, scales, scale_sem.at[0]).start()
    for q in range(2 * chunks):
        pltpu.make_async_copy(codes.at[:, pl.ds(chunk_column(q), LANES)], cbuf.at[q], code_sem.at[0]).start()

    pl.semaphore_wait(barrier, CORES + 3 + jnp.where(jnp.logical_and(near, half == 1), CORES, 0))

    def remote(src, dst, send, recv, **device):
        return pltpu.make_async_remote_copy(
            src_ref=src, dst_ref=dst, send_sem=send, recv_sem=recv, device_id=device, device_id_type=MESH)

    def mate_copy():
        return remote(pbuf.at[rows_of(s)], pbuf.at[rows_of(s)], p_send.at[0], mate_recv.at[0], seq=beside_device)

    def start_kv(to):
        def one(unit, _):
            k, which = unit // 2, lax.rem(unit, 2)
            remote(
                own.at[which, :, owned_chunk(to, k)], kv.at[k, which, all_rows_of(s)],
                kv_send.at[0], kv_recv.at[k], seq=to).start()
            return 0

        return one

    def start_chip(chip, low, high):
        def both(unit, _):
            for c in range(CORES):
                start_kv(chip * CORES + c)(unit, 0)
            return 0

        lax.fori_loop(low, high, both, 0)

    early_units = jnp.where(half == 0, 3, 2)

    def beside(low, high):
        start_chip(beside_chip, low, high)

    @pl.when(near)
    def _():
        drain(own, own_sem.at[1])
        start_chip(across(0), 0, 2 * chunks)

        @pl.when(half == 0)
        def _():
            pl.semaphore_wait(met.at[1], CORES)

        greet(met.at[0], beside_chip)
        greet(met.at[2], across(0))
        drain(pbuf.at[rows_of(s)], own_sem.at[0])
        mate_copy().start()

    @pl.when(far)
    def _():
        pl.when(half == 0)(lambda: greet(met.at[1], beside_chip))
        drain(pbuf.at[rows_of(s)], own_sem.at[0])
        mate_copy().start()

    for k in range(chunks):
        for which, src in enumerate((key, value)):
            pltpu.make_async_copy(
                src.at[:, owned_chunk(s, k)], kv.at[k, which, all_rows_of(s)], kv_recv.at[k]).start()
    pltpu.make_async_copy(query_gain_in, gains.at[0], gain_sem.at[0]).start()
    pltpu.make_async_copy(key_gain_in, gains.at[1], gain_sem.at[0]).start()

    def weight_copy(pair, recv, start, size, to):
        at = pl.ds(pl.multiple_of(start, size), size)
        return remote(wbuf.at[pair, at], wbuf.at[pair, at], w_send.at[0], recv.at[pair], fsdp=to)

    part = rows // 2

    def weights_out(pair):
        for recv, row_half in ((first_recv, 0), (rest_w_recv, part)):
            weight_copy(pair, recv, f * rows + row_half, part, row_mate).start()
            weight_copy(pair, recv, f * rows + part - row_half, part, column_mate).start()

    def relay(pair):
        drain(wbuf.at[pair, pl.ds(0, rows)], first_recv.at[pair])
        weight_copy(pair, rest_w_recv, row_mate * rows, part, column_mate).start()
        weight_copy(pair, rest_w_recv, column_mate * rows + part, part, row_mate).start()

    drain(scales, scale_sem.at[0])
    drain(cbuf, code_sem.at[0])

    def dequantize_pair(pair, _):
        for side in range(2):
            q = 2 * pair + side
            for block in range(rows // BLOCK):
                scale = scales[block, chunk_column(q) // BLOCK]
                piece = cbuf[q, block * BLOCK:(block + 1) * BLOCK, :].astype(jnp.float32) * scale
                at = pl.ds(pl.multiple_of(f * rows + block * BLOCK, BLOCK), BLOCK)
                wbuf[pair, at, side * LANES:(side + 1) * LANES] = piece.astype(jnp.bfloat16)

        pl.when(pair == 0)(lambda: weights_out(0))
        return 0

    lax.fori_loop(0, chunks, dequantize_pair, 0)

    @pl.when(near)
    def _():
        pl.semaphore_wait(met.at[2], CORES)
        greet(met.at[3], beside_chip)

    @pl.when(far)
    def _():
        drain(own, own_sem.at[1])
        pl.semaphore_wait(met.at[0], CORES)
        start_chip(across(0), 0, 2 * chunks)
        beside(0, early_units)
        pl.semaphore_wait(met.at[3], CORES)

    start_chip(across(1), 0, 2 * chunks)
    remote(pbuf.at[rows_of(s)], pbuf.at[rows_of(s)], p_send.at[0], partner_recv.at[0], seq=partner).start()
    lax.fori_loop(0, 2 * chunks, start_kv(partner), 0)

    def forward():
        at = rows_of(beside_device)
        drain(pbuf.at[at], mate_recv.at[0])
        remote(pbuf.at[at], pbuf.at[at], p_send.at[0], rest_recv.at[0], seq=partner).start()

    other = lax.rem(s + m, n)
    tile = CORES * tokens
    own_start = pl.multiple_of(place // CORES * tile, tile)
    beside_start = pl.multiple_of(beside_device // CORES * tile - half * group, tile)

    def project(pair, start, size):
        at = pl.ds(start, size)
        there = pl.ds(pl.multiple_of(half * group + start, tile), size)
        both = jnp.dot(pbuf[at, :], wbuf[pair], preferred_element_type=jnp.float32)
        for side in range(2):
            q = 2 * pair + side
            normed = column_norm(
                both[:, side * LANES:(side + 1) * LANES], gains[0, :, pl.ds(chunk_column(q), LANES)])
            if q < chunks:
                qsend[q, at] = normed
                remote(qsend.at[q, at], qbuf.at[q, there], q_send.at[0], q_recv.at[q], seq=other).start()
            else:
                qbuf[q - chunks, there] = normed

    def weights_in(pair):
        drain(wbuf.at[pair, pl.ds(0, 2 * rows)], rest_w_recv.at[pair])

    relay(0)
    weights_out(1)
    drain(gains, gain_sem.at[0])
    drain(pbuf.at[rows_of(s)], partner_recv.at[0])
    weights_in(0)
    project(0, own_start, tile)
    pl.when(near)(forward)
    for pair in range(1, chunks - 1):
        relay(pair)
        weights_out(pair + 1)
    pl.when(far)(forward)
    drain(pbuf.at[rows_of(s)], rest_recv.at[0])
    project(0, beside_start, tile)
    for pair in range(1, chunks - 1):
        weights_in(pair)
        project(pair, 0, group)
    beside(jnp.where(far, early_units, 0), 2 * chunks)
    relay(chunks - 1)
    weights_in(chunks - 1)
    project(chunks - 1, 0, group)

    exponent = HDIM ** (-0.5) * math.log2(math.e)

    def out_copy(k, to):
        return remote(obuf.at[k, all_rows_of(to)], out.at[:, owned_chunk(s, k)], o_send.at[0], o_recv.at[0], seq=to)

    first = lax.broadcasted_iota(jnp.int32, (tile, LANES), 1) < HDIM

    order = attend_order(chunks, chips)

    def entry(step, column):
        return sum(jnp.where(step == at, row[column], 0) for at, row in enumerate(order))

    def attend_step(step, _):
        mine, k, i, opens = (entry(step, column) for column in range(4))
        own_side = half * chips + lax.rem(place // CORES + 1 + i, chips)
        chip = jnp.where(mine == 1, own_side, across(chips - 1 - i))
        here = pl.ds(pl.multiple_of(chip * tile, tile), tile)

        @pl.when(opens == 1)
        def _():
            drain(kv.at[k], kv_recv.at[k])
            kv[k, 0] = column_norm(kv[k, 0].astype(jnp.float32), gains[1, :, owned_chunk(s, k)])
            drain(qsend.at[k], q_recv.at[k])

        values = kv[k, 1]
        keys = kv[k, 0]
        queries = qbuf[k, here]
        results = []
        for mask in (first, jnp.logical_not(first)):
            masked = jnp.where(mask, queries, jnp.zeros_like(queries))
            scores = lax.dot_general(
                masked, keys, (((1,), (1,)), ((), ())), preferred_element_type=jnp.float32)
            largest = jnp.max(scores, axis=-1, keepdims=True)
            probability = jnp.exp2((scores - largest) * exponent)
            normaliser = jnp.sum(probability, axis=-1, keepdims=True)
            blended = jnp.dot(
                probability.astype(jnp.bfloat16), values, preferred_element_type=jnp.float32)
            results.append(blended / normaliser)
        obuf[k, here] = jnp.where(first, results[0], results[1]).astype(jnp.bfloat16)
        for c in range(CORES):
            to = chip * CORES + c

            @pl.when(to != s)
            def _():
                out_copy(k, to).start()

            @pl.when(to == s)
            def _():
                out[:, owned_chunk(s, k)] = obuf[k, all_rows_of(s)]

        return 0

    lax.fori_loop(0, len(order), attend_step, 0)

    drain(pbuf.at[pl.ds(0, (2 * chips - 1) * tokens)], p_send.at[0])
    drain(wbuf.at[:, pl.ds(0, 3 * rows)], w_send.at[0])
    drain(kv.at[:, :, pl.ds(0, (n - 1) * tokens)], kv_send.at[0])
    drain(qsend, q_send.at[0])
    drain(obuf.at[:, pl.ds(0, (n - 1) * tokens)], o_send.at[0])
    drain(out.at[:, pl.ds(0, (n - 1) * width)], o_recv.at[0])


def fused_per_device(n, fn, patches, weight_codes, block_scales, key_proj, value_proj, query_gain, key_gain):
    _, tokens, features = patches.shape
    rows, columns = weight_codes.shape
    width = columns // n
    chunks = width // LANES
    group = n // 2 * tokens
    chips = n // 2 // CORES
    bf16 = jnp.bfloat16
    dma = pltpu.SemaphoreType.DMA
    anywhere = pl.BlockSpec(memory_space=pl.ANY)
    result = pl.pallas_call(
        functools.partial(fused_kernel, n, fn),
        out_shape=pltpu.VMEM((tokens, columns), bf16),
        in_specs=[anywhere] * 7,
        out_specs=pl.BlockSpec(memory_space=pltpu.VMEM),
        scratch_shapes=[
            pltpu.VMEM((group, features), bf16),
            pltpu.VMEM((2 * chunks, rows, LANES), jnp.int32),
            pltpu.VMEM((chunks, features, 2 * LANES), bf16),
            pltpu.VMEM((2, tokens, columns), bf16),
            pltpu.VMEM((chunks, 2, n * tokens, LANES), bf16),
            pltpu.VMEM((chunks, group, LANES), bf16),
            pltpu.VMEM((chunks, n * tokens, LANES), bf16),
            pltpu.VMEM((chunks, n * tokens, LANES), bf16),
            pltpu.VMEM((2, 1, columns), jnp.float32),
            pltpu.SMEM(block_scales.shape, jnp.float32),
            dma((2,)), dma((1,)), dma((1,)), dma((1,)), dma((1,)), dma((1,)), dma((1,)), dma((1,)),
            dma((chunks,)), dma((chunks,)), dma((1,)),
            dma((1,)), dma((chunks,)), dma((1,)), dma((chunks,)), dma((1,)), dma((1,)),
            pltpu.SemaphoreType.REGULAR((4,)),
        ],
        compiler_params=pltpu.CompilerParams(
            collective_id=0, has_side_effects=True, vmem_limit_bytes=56 * 1024 * 1024),
    )(
        patches.reshape(tokens, features), weight_codes, block_scales,
        key_proj.reshape(tokens, columns), value_proj.reshape(tokens, columns),
        query_gain.reshape(1, columns), key_gain.reshape(1, columns),
    )
    return result.reshape(1, tokens, columns)


def solution(mesh):
    n, fn = mesh.shape["seq"], mesh.shape["fsdp"]
    specs = (
        P("fsdp", "seq", None), P("fsdp", None), P("fsdp", None),
        P("fsdp", "seq", None), P("fsdp", "seq", None), P(), P(),
    )

    def whole(*arrays):
        patches, weight_codes = arrays[:2]
        fits = patches.shape[0] == fn == GRID * GRID and weight_codes.shape[1] % (n * LANES) == 0 and n == 2 * GRID * CORES
        body = functools.partial(fused_per_device, n, fn) if fits else per_device
        return jax.shard_map(
            body, mesh=mesh, in_specs=specs, out_specs=P("fsdp", "seq", None), check_vma=False
        )(*arrays)

    return whole
```

```python
import functools
import math
import jax
import jax.numpy as jnp
from jax import lax
from jax.experimental import pallas as pl
from jax.experimental.pallas import tpu as pltpu
from jax.sharding import PartitionSpec as P

HEADS = 48
HDIM = 64
BLOCK = 128


NORM_FLOOR = 0.25


def head_norm(projected, gain_row):
    shaped = projected.reshape(projected.shape[:-1] + (HEADS, HDIM))
    average = jnp.mean(shaped, axis=-1, keepdims=True)
    centred = shaped - average
    spread = jnp.mean(centred * centred, axis=-1, keepdims=True)
    normed = centred * lax.rsqrt(spread + NORM_FLOOR) * gain_row.reshape(HEADS, HDIM)
    return normed.astype(jnp.bfloat16)


def dequantize(weight_codes, block_scales):
    row_count, column_count = weight_codes.shape
    blocked = weight_codes.astype(jnp.float32).reshape(
        row_count // BLOCK, BLOCK, column_count // BLOCK, BLOCK
    )
    return (
        (blocked * block_scales[:, None, :, None])
        .reshape(row_count, column_count)
        .astype(jnp.bfloat16)
    )


def start_of(query_view):
    image_count, token_count, head_count = (
        query_view.shape[0],
        query_view.shape[1],
        query_view.shape[2],
    )
    return (
        jnp.full((image_count, token_count, head_count), -1e30, jnp.float32),
        jnp.zeros((image_count, token_count, head_count), jnp.float32),
        jnp.zeros(query_view.shape, jnp.float32),
    )


def attend_block(query_view, state_now, key_view, value_view):
    running_max, running_sum, weighted = state_now
    scores = jnp.einsum(
        "ithd,ishd->iths", query_view, key_view, preferred_element_type=jnp.float32
    ) * HDIM ** (-0.5)
    newest = jnp.maximum(running_max, jnp.max(scores, axis=-1))
    probability = jnp.exp(scores - newest[..., None])
    running_sum = jnp.sum(probability, axis=-1)
    blended = jnp.einsum(
        "iths,ishd->ithd",
        probability.astype(jnp.bfloat16),
        value_view,
        preferred_element_type=jnp.float32,
    )
    weighted = blended
    return (newest, running_sum, weighted)


def per_device(patches, weight_codes, block_scales, key_proj, value_proj, query_gain, key_gain):
    image_count, token_count, feature_count = patches.shape
    flat_rows = patches.reshape(image_count * token_count, feature_count)
    key_norm = head_norm(key_proj.astype(jnp.float32), key_gain)
    value_view = value_proj.reshape(image_count, token_count, HEADS, HDIM)
    local_weight = dequantize(weight_codes, block_scales)
    group_rows = lax.all_to_all(flat_rows, "fsdp", split_axis=1, concat_axis=0, tiled=True)
    queries = lax.psum_scatter(
        jnp.dot(group_rows, local_weight, preferred_element_type=jnp.float32),
        "fsdp",
        scatter_dimension=0,
        tiled=True,
    )
    query_view = head_norm(queries, query_gain).reshape(image_count, token_count, HEADS, HDIM)
    finished = attend_block(
        query_view,
        start_of(query_view),
        lax.all_gather(key_norm, "seq", axis=1, tiled=True),
        lax.all_gather(value_view, "seq", axis=1, tiled=True),
    )
    attended = finished[2] / finished[1][..., None]
    return attended.reshape(image_count, token_count, HEADS * HDIM).astype(jnp.bfloat16)


MESH = pl.DeviceIdType.MESH
LANES = 128
CORES = 2
GRID = 2


def column_norm(values, gain_row):
    lane = lambda axis: lax.broadcasted_iota(jnp.int32, (LANES, LANES), axis) < HDIM
    spread_out = jnp.where(lane(0) == lane(1), 1.0 / HDIM, 0.0).astype(jnp.bfloat16)
    spread_out = jnp.concatenate([spread_out, spread_out], axis=0)

    def mean_of(t):
        high = t.astype(jnp.bfloat16)
        low = (t - high.astype(jnp.float32)).astype(jnp.bfloat16)
        return jnp.dot(jnp.concatenate([high, low], axis=1), spread_out, preferred_element_type=jnp.float32)

    centred = values - mean_of(values)
    normed = centred * lax.rsqrt(mean_of(centred * centred) + NORM_FLOOR) * gain_row
    return normed.astype(jnp.bfloat16)


def attend_order(chunks, chips):
    order, late = [], []
    for k in range(chunks):
        order += [(0, k, i, int(i == 0)) for i in range(chips if k == 0 else 1)]
        order += late
        late = [(0, k, i, 0) for i in range(1, chips)] if k > 0 else []
        if k == chunks - 1:
            order += late
        order += [(1, k, i, 0) for i in range(chips)]
    return order


def fused_kernel(
    n, fn, patches, codes, scales_in, key, value, query_gain_in, key_gain_in, out,
    pbuf, cbuf, wbuf, own, kv, qsend, qbuf, obuf, gains, scales,
    own_sem, code_sem, scale_sem, gain_sem, mate_recv, partner_recv, rest_recv, p_send, first_recv, rest_w_recv, w_send,
    kv_send, kv_recv, q_send, q_recv, o_send, o_recv, met,
):
    s, f = lax.axis_index("seq"), lax.axis_index("fsdp")
    m = n // 2
    half, place = s // m, lax.rem(s, m)
    tokens = patches.shape[0]
    rows, columns = codes.shape
    width = columns // n
    chunks = width // LANES
    group = m * tokens
    chips = m // CORES
    core = lax.rem(s, CORES)
    partner = s + 1 - 2 * core

    barrier = pltpu.get_barrier_semaphore()
    far = place // CORES == jnp.where(half == 0, 0, chips - 1)
    near = jnp.logical_not(far)
    row_mate = f + 1 - 2 * lax.rem(f, GRID)
    column_mate = lax.rem(f + GRID, fn)

    beside_device = half * m + lax.rem(place + CORES, m)
    def across(j):
        return jnp.where(half == 0, chips + j, chips - 1 - j)

    def greet(semaphore, chip):
        for c in range(CORES):
            pl.semaphore_signal(semaphore, inc=1, device_id={"seq": chip * CORES + c}, device_id_type=MESH)

    beside_chip = beside_device // CORES

    @pl.when(near)
    def _():
        greet(barrier, across(0))
        greet(barrier, beside_chip)

    @pl.when(jnp.logical_and(far, half == 1))
    def _():
        greet(barrier, beside_chip)

    pl.semaphore_signal(barrier, inc=1, device_id={"seq": partner}, device_id_type=MESH)
    for mate in (row_mate, column_mate):
        pl.semaphore_signal(barrier, inc=1, device_id={"fsdp": mate}, device_id_type=MESH)

    def rows_of(device):
        return pl.ds(pl.multiple_of(lax.rem(device, m) * tokens, tokens), tokens)

    def all_rows_of(device):
        return pl.ds(pl.multiple_of(device * tokens, tokens), tokens)

    def owned(device):
        return pl.multiple_of((lax.rem(device, m) * 2 + device // m) * width, LANES)

    def owned_chunk(device, k):
        return pl.ds(pl.multiple_of(owned(device) + k * LANES, LANES), LANES)

    def chunk_column(q):
        side = jnp.where(q < chunks, 1 - half, half)
        return pl.multiple_of((place * 2 + side) * width + lax.rem(q, chunks) * LANES, LANES)

    def drain(ref, sem):
        pltpu.make_async_copy(ref, ref, sem).wait()

    pltpu.make_async_copy(patches, pbuf.at[rows_of(s)], own_sem.at[0]).start()
    for which, src in enumerate((key, value)):
        pltpu.make_async_copy(src, own.at[which], own_sem.at[1]).start()
    pltpu.make_async_copy(scales_in, scales, scale_sem.at[0]).start()
    for q in range(2 * chunks):
        pltpu.make_async_copy(codes.at[:, pl.ds(chunk_column(q), LANES)], cbuf.at[q], code_sem.at[0]).start()

    pl.semaphore_wait(barrier, CORES + 3 + jnp.where(jnp.logical_and(near, half == 1), CORES, 0))

    def remote(src, dst, send, recv, **device):
        return pltpu.make_async_remote_copy(
            src_ref=src, dst_ref=dst, send_sem=send, recv_sem=recv, device_id=device, device_id_type=MESH)

    def mate_copy():
        return remote(pbuf.at[rows_of(s)], pbuf.at[rows_of(s)], p_send.at[0], mate_recv.at[0], seq=beside_device)

    def start_kv(to):
        def one(k, _):
            remote(
                own.at[:, :, owned_chunk(to, k)], kv.at[k, :, all_rows_of(s)],
                kv_send.at[0], kv_recv.at[k], seq=to).start()
            return 0

        return one

    def start_chip(chip, low, high):
        def both(k, _):
            for c in range(CORES):
                start_kv(chip * CORES + c)(k, 0)
            return 0

        lax.fori_loop(low, high, both, 0)

    def beside(low, high):
        start_chip(beside_chip, low, high)

    @pl.when(near)
    def _():
        drain(own, own_sem.at[1])
        start_chip(across(0), 0, chunks)

        @pl.when(half == 0)
        def _():
            pl.semaphore_wait(met.at[1], CORES)

        greet(met.at[0], beside_chip)
        greet(met.at[2], across(0))
        drain(pbuf.at[rows_of(s)], own_sem.at[0])
        mate_copy().start()

    @pl.when(far)
    def _():
        pl.when(half == 0)(lambda: greet(met.at[1], beside_chip))
        drain(pbuf.at[rows_of(s)], own_sem.at[0])
        mate_copy().start()

    for k in range(chunks):
        for which, src in enumerate((key, value)):
            pltpu.make_async_copy(
                src.at[:, owned_chunk(s, k)], kv.at[k, which, all_rows_of(s)], kv_recv.at[k]).start()
    pltpu.make_async_copy(query_gain_in, gains.at[0], gain_sem.at[0]).start()
    pltpu.make_async_copy(key_gain_in, gains.at[1], gain_sem.at[0]).start()

    def weight_copy(pair, recv, start, size, to):
        at = pl.ds(pl.multiple_of(start, size), size)
        return remote(wbuf.at[pair, at], wbuf.at[pair, at], w_send.at[0], recv.at[pair], fsdp=to)

    part = rows // 2

    def weights_out(pair):
        for recv, row_half in ((first_recv, 0), (rest_w_recv, part)):
            weight_copy(pair, recv, f * rows + row_half, part, row_mate).start()
            weight_copy(pair, recv, f * rows + part - row_half, part, column_mate).start()

    def relay(pair):
        drain(wbuf.at[pair, pl.ds(0, rows)], first_recv.at[pair])
        weight_copy(pair, rest_w_recv, row_mate * rows, part, column_mate).start()
        weight_copy(pair, rest_w_recv, column_mate * rows + part, part, row_mate).start()

    drain(scales, scale_sem.at[0])
    drain(cbuf, code_sem.at[0])

    def dequantize_pair(pair, _):
        for side in range(2):
            q = 2 * pair + side
            for block in range(rows // BLOCK):
                scale = scales[block, chunk_column(q) // BLOCK]
                piece = cbuf[q, block * BLOCK:(block + 1) * BLOCK, :].astype(jnp.float32) * scale
                at = pl.ds(pl.multiple_of(f * rows + block * BLOCK, BLOCK), BLOCK)
                wbuf[pair, at, side * LANES:(side + 1) * LANES] = piece.astype(jnp.bfloat16)

        pl.when(pair == 0)(lambda: weights_out(0))
        return 0

    lax.fori_loop(0, chunks, dequantize_pair, 0)

    @pl.when(near)
    def _():
        pl.semaphore_wait(met.at[2], CORES)
        greet(met.at[3], beside_chip)

    @pl.when(far)
    def _():
        drain(own, own_sem.at[1])
        pl.semaphore_wait(met.at[0], CORES)
        start_chip(across(0), 0, chunks)
        beside(0, 1)
        pl.semaphore_wait(met.at[3], CORES)

    start_chip(across(1), 0, chunks)
    remote(pbuf.at[rows_of(s)], pbuf.at[rows_of(s)], p_send.at[0], partner_recv.at[0], seq=partner).start()
    lax.fori_loop(0, chunks, start_kv(partner), 0)

    def forward():
        at = rows_of(beside_device)
        drain(pbuf.at[at], mate_recv.at[0])
        remote(pbuf.at[at], pbuf.at[at], p_send.at[0], rest_recv.at[0], seq=partner).start()

    other = lax.rem(s + m, n)
    tile = CORES * tokens
    own_start = pl.multiple_of(place // CORES * tile, tile)
    beside_start = pl.multiple_of(beside_device // CORES * tile - half * group, tile)

    def project(pair, start, size):
        at = pl.ds(start, size)
        there = pl.ds(pl.multiple_of(half * group + start, tile), size)
        both = jnp.dot(pbuf[at, :], wbuf[pair], preferred_element_type=jnp.float32)
        for side in range(2):
            q = 2 * pair + side
            normed = column_norm(
                both[:, side * LANES:(side + 1) * LANES], gains[0, :, pl.ds(chunk_column(q), LANES)])
            if q < chunks:
                qsend[q, at] = normed
                remote(qsend.at[q, at], qbuf.at[q, there], q_send.at[0], q_recv.at[q], seq=other).start()
            else:
                qbuf[q - chunks, there] = normed

    def weights_in(pair):
        drain(wbuf.at[pair, pl.ds(0, 2 * rows)], rest_w_recv.at[pair])

    relay(0)
    weights_out(1)
    drain(gains, gain_sem.at[0])
    drain(pbuf.at[rows_of(s)], partner_recv.at[0])
    weights_in(0)
    project(0, own_start, tile)
    pl.when(near)(forward)
    for pair in range(1, chunks - 1):
        relay(pair)
        weights_out(pair + 1)
    pl.when(far)(forward)
    drain(pbuf.at[rows_of(s)], rest_recv.at[0])
    project(0, beside_start, tile)
    for pair in range(1, chunks - 1):
        weights_in(pair)
        project(pair, 0, group)
    beside(jnp.where(far, 1, 0), chunks)
    relay(chunks - 1)
    weights_in(chunks - 1)
    project(chunks - 1, 0, group)

    exponent = HDIM ** (-0.5) * math.log2(math.e)

    def out_copy(k, to):
        return remote(obuf.at[k, all_rows_of(to)], out.at[:, owned_chunk(s, k)], o_send.at[0], o_recv.at[0], seq=to)

    first = lax.broadcasted_iota(jnp.int32, (tile, LANES), 1) < HDIM

    order = attend_order(chunks, chips)

    def entry(step, column):
        return sum(jnp.where(step == at, row[column], 0) for at, row in enumerate(order))

    def attend_step(step, _):
        mine, k, i, opens = (entry(step, column) for column in range(4))
        own_side = half * chips + lax.rem(place // CORES + 1 + i, chips)
        chip = jnp.where(mine == 1, own_side, across(chips - 1 - i))
        here = pl.ds(pl.multiple_of(chip * tile, tile), tile)

        @pl.when(opens == 1)
        def _():
            drain(kv.at[k], kv_recv.at[k])
            kv[k, 0] = column_norm(kv[k, 0].astype(jnp.float32), gains[1, :, owned_chunk(s, k)])
            drain(qsend.at[k], q_recv.at[k])

        values = kv[k, 1]
        keys = kv[k, 0]
        queries = qbuf[k, here]
        results = []
        for mask in (first, jnp.logical_not(first)):
            masked = jnp.where(mask, queries, jnp.zeros_like(queries))
            scores = lax.dot_general(
                masked, keys, (((1,), (1,)), ((), ())), preferred_element_type=jnp.float32)
            largest = jnp.max(scores, axis=-1, keepdims=True)
            probability = jnp.exp2((scores - largest) * exponent)
            normaliser = jnp.sum(probability, axis=-1, keepdims=True)
            blended = jnp.dot(
                probability.astype(jnp.bfloat16), values, preferred_element_type=jnp.float32)
            results.append(blended / normaliser)
        obuf[k, here] = jnp.where(first, results[0], results[1]).astype(jnp.bfloat16)
        for c in range(CORES):
            to = chip * CORES + c

            @pl.when(to != s)
            def _():
                out_copy(k, to).start()

            @pl.when(to == s)
            def _():
                out[:, owned_chunk(s, k)] = obuf[k, all_rows_of(s)]

        return 0

    lax.fori_loop(0, len(order), attend_step, 0)

    drain(pbuf.at[pl.ds(0, (2 * chips - 1) * tokens)], p_send.at[0])
    drain(wbuf.at[:, pl.ds(0, 3 * rows)], w_send.at[0])
    drain(kv.at[:, :, pl.ds(0, (n - 1) * tokens)], kv_send.at[0])
    drain(qsend, q_send.at[0])
    drain(obuf.at[:, pl.ds(0, (n - 1) * tokens)], o_send.at[0])
    drain(out.at[:, pl.ds(0, (n - 1) * width)], o_recv.at[0])


def fused_per_device(n, fn, patches, weight_codes, block_scales, key_proj, value_proj, query_gain, key_gain):
    _, tokens, features = patches.shape
    rows, columns = weight_codes.shape
    width = columns // n
    chunks = width // LANES
    group = n // 2 * tokens
    chips = n // 2 // CORES
    bf16 = jnp.bfloat16
    dma = pltpu.SemaphoreType.DMA
    anywhere = pl.BlockSpec(memory_space=pl.ANY)
    result = pl.pallas_call(
        functools.partial(fused_kernel, n, fn),
        out_shape=pltpu.VMEM((tokens, columns), bf16),
        in_specs=[anywhere] * 7,
        out_specs=pl.BlockSpec(memory_space=pltpu.VMEM),
        scratch_shapes=[
            pltpu.VMEM((group, features), bf16),
            pltpu.VMEM((2 * chunks, rows, LANES), jnp.int32),
            pltpu.VMEM((chunks, features, 2 * LANES), bf16),
            pltpu.VMEM((2, tokens, columns), bf16),
            pltpu.VMEM((chunks, 2, n * tokens, LANES), bf16),
            pltpu.VMEM((chunks, group, LANES), bf16),
            pltpu.VMEM((chunks, n * tokens, LANES), bf16),
            pltpu.VMEM((chunks, n * tokens, LANES), bf16),
            pltpu.VMEM((2, 1, columns), jnp.float32),
            pltpu.SMEM(block_scales.shape, jnp.float32),
            dma((2,)), dma((1,)), dma((1,)), dma((1,)), dma((1,)), dma((1,)), dma((1,)), dma((1,)),
            dma((chunks,)), dma((chunks,)), dma((1,)),
            dma((1,)), dma((chunks,)), dma((1,)), dma((chunks,)), dma((1,)), dma((1,)),
            pltpu.SemaphoreType.REGULAR((4,)),
        ],
        compiler_params=pltpu.CompilerParams(
            collective_id=0, has_side_effects=True, vmem_limit_bytes=56 * 1024 * 1024),
    )(
        patches.reshape(tokens, features), weight_codes, block_scales,
        key_proj.reshape(tokens, columns), value_proj.reshape(tokens, columns),
        query_gain.reshape(1, columns), key_gain.reshape(1, columns),
    )
    return result.reshape(1, tokens, columns)


def solution(mesh):
    n, fn = mesh.shape["seq"], mesh.shape["fsdp"]
    specs = (
        P("fsdp", "seq", None), P("fsdp", None), P("fsdp", None),
        P("fsdp", "seq", None), P("fsdp", "seq", None), P(), P(),
    )

    def whole(*arrays):
        patches, weight_codes = arrays[:2]
        fits = patches.shape[0] == fn == GRID * GRID and weight_codes.shape[1] % (n * LANES) == 0 and n == 2 * GRID * CORES
        body = functools.partial(fused_per_device, n, fn) if fits else per_device
        return jax.shard_map(
            body, mesh=mesh, in_specs=specs, out_specs=P("fsdp", "seq", None), check_vma=False
        )(*arrays)

    return whole
```

```python
import functools
import math
import jax
import jax.numpy as jnp
from jax import lax
from jax.experimental import pallas as pl
from jax.experimental.pallas import tpu as pltpu
from jax.sharding import PartitionSpec as P

HEADS = 48
HDIM = 64
BLOCK = 128


NORM_FLOOR = 0.25


def head_norm(projected, gain_row):
    shaped = projected.reshape(projected.shape[:-1] + (HEADS, HDIM))
    average = jnp.mean(shaped, axis=-1, keepdims=True)
    centred = shaped - average
    spread = jnp.mean(centred * centred, axis=-1, keepdims=True)
    normed = centred * lax.rsqrt(spread + NORM_FLOOR) * gain_row.reshape(HEADS, HDIM)
    return normed.astype(jnp.bfloat16)


def dequantize(weight_codes, block_scales):
    row_count, column_count = weight_codes.shape
    blocked = weight_codes.astype(jnp.float32).reshape(
        row_count // BLOCK, BLOCK, column_count // BLOCK, BLOCK
    )
    return (
        (blocked * block_scales[:, None, :, None])
        .reshape(row_count, column_count)
        .astype(jnp.bfloat16)
    )


def start_of(query_view):
    image_count, token_count, head_count = (
        query_view.shape[0],
        query_view.shape[1],
        query_view.shape[2],
    )
    return (
        jnp.full((image_count, token_count, head_count), -1e30, jnp.float32),
        jnp.zeros((image_count, token_count, head_count), jnp.float32),
        jnp.zeros(query_view.shape, jnp.float32),
    )


def attend_block(query_view, state_now, key_view, value_view):
    running_max, running_sum, weighted = state_now
    scores = jnp.einsum(
        "ithd,ishd->iths", query_view, key_view, preferred_element_type=jnp.float32
    ) * HDIM ** (-0.5)
    newest = jnp.maximum(running_max, jnp.max(scores, axis=-1))
    probability = jnp.exp(scores - newest[..., None])
    running_sum = jnp.sum(probability, axis=-1)
    blended = jnp.einsum(
        "iths,ishd->ithd",
        probability.astype(jnp.bfloat16),
        value_view,
        preferred_element_type=jnp.float32,
    )
    weighted = blended
    return (newest, running_sum, weighted)


def per_device(patches, weight_codes, block_scales, key_proj, value_proj, query_gain, key_gain):
    image_count, token_count, feature_count = patches.shape
    flat_rows = patches.reshape(image_count * token_count, feature_count)
    key_norm = head_norm(key_proj.astype(jnp.float32), key_gain)
    value_view = value_proj.reshape(image_count, token_count, HEADS, HDIM)
    local_weight = dequantize(weight_codes, block_scales)
    group_rows = lax.all_to_all(flat_rows, "fsdp", split_axis=1, concat_axis=0, tiled=True)
    queries = lax.psum_scatter(
        jnp.dot(group_rows, local_weight, preferred_element_type=jnp.float32),
        "fsdp",
        scatter_dimension=0,
        tiled=True,
    )
    query_view = head_norm(queries, query_gain).reshape(image_count, token_count, HEADS, HDIM)
    finished = attend_block(
        query_view,
        start_of(query_view),
        lax.all_gather(key_norm, "seq", axis=1, tiled=True),
        lax.all_gather(value_view, "seq", axis=1, tiled=True),
    )
    attended = finished[2] / finished[1][..., None]
    return attended.reshape(image_count, token_count, HEADS * HDIM).astype(jnp.bfloat16)


MESH = pl.DeviceIdType.MESH
LANES = 128
CORES = 2
GRID = 2


def column_norm(values, gain_row):
    lane = lambda axis: lax.broadcasted_iota(jnp.int32, (LANES, LANES), axis) < HDIM
    spread_out = jnp.where(lane(0) == lane(1), 1.0 / HDIM, 0.0).astype(jnp.bfloat16)
    spread_out = jnp.concatenate([spread_out, spread_out], axis=0)

    def mean_of(t):
        high = t.astype(jnp.bfloat16)
        low = (t - high.astype(jnp.float32)).astype(jnp.bfloat16)
        return jnp.dot(jnp.concatenate([high, low], axis=1), spread_out, preferred_element_type=jnp.float32)

    centred = values - mean_of(values)
    normed = centred * lax.rsqrt(mean_of(centred * centred) + NORM_FLOOR) * gain_row
    return normed.astype(jnp.bfloat16)


def attend_order(chunks, chips):
    order, late = [], []
    for k in range(chunks):
        order += [(0, k, i, int(i == 0)) for i in range(chips if k == 0 else 1)]
        order += late
        late = [(0, k, i, 0) for i in range(1, chips)] if k > 0 else []
        if k == chunks - 1:
            order += late
        order += [(1, k, i, 0) for i in range(chips)]
    return order


def fused_kernel(
    n, fn, patches, codes, scales_in, key, value, query_gain_in, key_gain_in, out,
    pbuf, cbuf, wbuf, own, kv, qsend, qbuf, obuf, gains, scales,
    own_sem, code_sem, scale_sem, gain_sem, mate_recv, partner_recv, rest_recv, p_send, first_recv, rest_w_recv, w_send,
    kv_send, kv_recv, q_send, q_recv, o_send, o_recv, met,
):
    s, f = lax.axis_index("seq"), lax.axis_index("fsdp")
    m = n // 2
    half, place = s // m, lax.rem(s, m)
    tokens = patches.shape[0]
    rows, columns = codes.shape
    width = columns // n
    chunks = width // LANES
    group = m * tokens
    chips = m // CORES
    core = lax.rem(s, CORES)
    partner = s + 1 - 2 * core

    barrier = pltpu.get_barrier_semaphore()
    far = place // CORES == jnp.where(half == 0, 0, chips - 1)
    near = jnp.logical_not(far)
    row_mate = f + 1 - 2 * lax.rem(f, GRID)
    column_mate = lax.rem(f + GRID, fn)

    beside_device = half * m + lax.rem(place + CORES, m)
    def across(j):
        return jnp.where(half == 0, chips + j, chips - 1 - j)

    def greet(semaphore, chip):
        for c in range(CORES):
            pl.semaphore_signal(semaphore, inc=1, device_id={"seq": chip * CORES + c}, device_id_type=MESH)

    beside_chip = beside_device // CORES

    @pl.when(near)
    def _():
        greet(barrier, across(0))
        greet(barrier, beside_chip)

    @pl.when(jnp.logical_and(far, half == 1))
    def _():
        greet(barrier, beside_chip)

    pl.semaphore_signal(barrier, inc=1, device_id={"seq": partner}, device_id_type=MESH)
    for mate in (row_mate, column_mate):
        pl.semaphore_signal(barrier, inc=1, device_id={"fsdp": mate}, device_id_type=MESH)

    def rows_of(device):
        return pl.ds(pl.multiple_of(lax.rem(device, m) * tokens, tokens), tokens)

    def all_rows_of(device):
        return pl.ds(pl.multiple_of(device * tokens, tokens), tokens)

    def owned(device):
        return pl.multiple_of((lax.rem(device, m) * 2 + device // m) * width, LANES)

    def owned_chunk(device, k):
        return pl.ds(pl.multiple_of(owned(device) + k * LANES, LANES), LANES)

    def chunk_column(q):
        side = jnp.where(q < chunks, 1 - half, half)
        return pl.multiple_of((place * 2 + side) * width + lax.rem(q, chunks) * LANES, LANES)

    def drain(ref, sem):
        pltpu.make_async_copy(ref, ref, sem).wait()

    pltpu.make_async_copy(patches, pbuf.at[rows_of(s)], own_sem.at[0]).start()
    for which, src in enumerate((key, value)):
        pltpu.make_async_copy(src, own.at[which], own_sem.at[1]).start()
    pltpu.make_async_copy(scales_in, scales, scale_sem.at[0]).start()
    for q in range(2 * chunks):
        pltpu.make_async_copy(codes.at[:, pl.ds(chunk_column(q), LANES)], cbuf.at[q], code_sem.at[0]).start()

    pl.semaphore_wait(barrier, CORES + 3 + jnp.where(jnp.logical_and(near, half == 1), CORES, 0))

    def remote(src, dst, send, recv, **device):
        return pltpu.make_async_remote_copy(
            src_ref=src, dst_ref=dst, send_sem=send, recv_sem=recv, device_id=device, device_id_type=MESH)

    def mate_copy():
        return remote(pbuf.at[rows_of(s)], pbuf.at[rows_of(s)], p_send.at[0], mate_recv.at[0], seq=beside_device)

    def start_kv(to):
        def one(k, _):
            remote(
                own.at[:, :, owned_chunk(to, k)], kv.at[k, :, all_rows_of(s)],
                kv_send.at[0], kv_recv.at[k], seq=to).start()
            return 0

        return one

    def start_chip(chip, low, high):
        def both(k, _):
            for c in range(CORES):
                start_kv(chip * CORES + c)(k, 0)
            return 0

        lax.fori_loop(low, high, both, 0)

    def beside(low, high):
        start_chip(beside_chip, low, high)

    @pl.when(near)
    def _():
        drain(own, own_sem.at[1])
        start_chip(across(0), 0, chunks)

        @pl.when(half == 0)
        def _():
            pl.semaphore_wait(met.at[1], CORES)

        greet(met.at[0], beside_chip)
        greet(met.at[2], across(0))
        drain(pbuf.at[rows_of(s)], own_sem.at[0])
        mate_copy().start()

    @pl.when(far)
    def _():
        pl.when(half == 0)(lambda: greet(met.at[1], beside_chip))
        drain(pbuf.at[rows_of(s)], own_sem.at[0])
        mate_copy().start()

    for k in range(chunks):
        for which, src in enumerate((key, value)):
            pltpu.make_async_copy(
                src.at[:, owned_chunk(s, k)], kv.at[k, which, all_rows_of(s)], kv_recv.at[k]).start()
    pltpu.make_async_copy(query_gain_in, gains.at[0], gain_sem.at[0]).start()
    pltpu.make_async_copy(key_gain_in, gains.at[1], gain_sem.at[0]).start()

    def weight_copy(pair, recv, start, size, to):
        at = pl.ds(pl.multiple_of(start, size), size)
        return remote(wbuf.at[pair, at], wbuf.at[pair, at], w_send.at[0], recv.at[pair], fsdp=to)

    part = rows // 2

    def weights_out(pair):
        for recv, row_half in ((first_recv, 0), (rest_w_recv, part)):
            weight_copy(pair, recv, f * rows + row_half, part, row_mate).start()
            weight_copy(pair, recv, f * rows + part - row_half, part, column_mate).start()

    def relay(pair):
        drain(wbuf.at[pair, pl.ds(0, rows)], first_recv.at[pair])
        weight_copy(pair, rest_w_recv, row_mate * rows, part, column_mate).start()
        weight_copy(pair, rest_w_recv, column_mate * rows + part, part, row_mate).start()

    drain(scales, scale_sem.at[0])
    drain(cbuf, code_sem.at[0])

    def dequantize_pair(pair, _):
        for side in range(2):
            q = 2 * pair + side
            for block in range(rows // BLOCK):
                scale = scales[block, chunk_column(q) // BLOCK]
                piece = cbuf[q, block * BLOCK:(block + 1) * BLOCK, :].astype(jnp.float32) * scale
                at = pl.ds(pl.multiple_of(f * rows + block * BLOCK, BLOCK), BLOCK)
                wbuf[pair, at, side * LANES:(side + 1) * LANES] = piece.astype(jnp.bfloat16)

        pl.when(pair == 0)(lambda: weights_out(0))
        return 0

    lax.fori_loop(0, chunks, dequantize_pair, 0)

    @pl.when(near)
    def _():
        pl.semaphore_wait(met.at[2], CORES)
        greet(met.at[3], beside_chip)

    @pl.when(far)
    def _():
        drain(own, own_sem.at[1])
        pl.semaphore_wait(met.at[0], CORES)
        start_chip(across(0), 0, chunks)
        beside(0, 1)
        pl.semaphore_wait(met.at[3], CORES)

    start_chip(across(1), 0, chunks)
    remote(pbuf.at[rows_of(s)], pbuf.at[rows_of(s)], p_send.at[0], partner_recv.at[0], seq=partner).start()
    lax.fori_loop(0, chunks, start_kv(partner), 0)

    def forward():
        at = rows_of(beside_device)
        drain(pbuf.at[at], mate_recv.at[0])
        remote(pbuf.at[at], pbuf.at[at], p_send.at[0], rest_recv.at[0], seq=partner).start()

    other = lax.rem(s + m, n)
    tile = CORES * tokens
    own_start = pl.multiple_of(place // CORES * tile, tile)
    beside_start = pl.multiple_of(beside_device // CORES * tile - half * group, tile)

    def project(pair, start, size):
        at = pl.ds(start, size)
        there = pl.ds(pl.multiple_of(half * group + start, tile), size)
        both = jnp.dot(pbuf[at, :], wbuf[pair], preferred_element_type=jnp.float32)
        for side in range(2):
            q = 2 * pair + side
            normed = column_norm(
                both[:, side * LANES:(side + 1) * LANES], gains[0, :, pl.ds(chunk_column(q), LANES)])
            if q < chunks:
                qsend[q, at] = normed
                remote(qsend.at[q, at], qbuf.at[q, there], q_send.at[0], q_recv.at[q], seq=other).start()
            else:
                qbuf[q - chunks, there] = normed

    def weights_in(pair):
        drain(wbuf.at[pair, pl.ds(0, 2 * rows)], rest_w_recv.at[pair])

    relay(0)
    weights_out(1)
    drain(gains, gain_sem.at[0])
    drain(pbuf.at[rows_of(s)], partner_recv.at[0])
    weights_in(0)
    project(0, own_start, tile)
    pl.when(near)(forward)
    for pair in range(1, chunks - 1):
        relay(pair)
        weights_out(pair + 1)
    pl.when(far)(forward)
    drain(pbuf.at[rows_of(s)], rest_recv.at[0])
    project(0, beside_start, tile)
    for pair in range(1, chunks - 1):
        weights_in(pair)
        project(pair, 0, group)
    beside(jnp.where(far, 1, 0), chunks)
    relay(chunks - 1)
    weights_in(chunks - 1)
    project(chunks - 1, 0, group)

    exponent = HDIM ** (-0.5) * math.log2(math.e)

    def out_copy(k, to):
        return remote(obuf.at[k, all_rows_of(to)], out.at[:, owned_chunk(s, k)], o_send.at[0], o_recv.at[0], seq=to)

    first = lax.broadcasted_iota(jnp.int32, (tile, LANES), 1) < HDIM

    order = attend_order(chunks, chips)

    def entry(step, column):
        return sum(jnp.where(step == at, row[column], 0) for at, row in enumerate(order))

    def attend_step(step, _):
        mine, k, i, opens = (entry(step, column) for column in range(4))
        own_side = half * chips + lax.rem(place // CORES + 1 + i, chips)
        chip = jnp.where(mine == 1, own_side, across(chips - 1 - i))
        here = pl.ds(pl.multiple_of(chip * tile, tile), tile)

        @pl.when(opens == 1)
        def _():
            drain(kv.at[k], kv_recv.at[k])
            kv[k, 0] = column_norm(kv[k, 0].astype(jnp.float32), gains[1, :, owned_chunk(s, k)])
            drain(qsend.at[k], q_recv.at[k])

        values = kv[k, 1]
        keys = kv[k, 0]
        queries = qbuf[k, here]
        results = []
        for mask in (first, jnp.logical_not(first)):
            masked = jnp.where(mask, queries, jnp.zeros_like(queries))
            scores = lax.dot_general(
                masked, keys, (((1,), (1,)), ((), ())), preferred_element_type=jnp.float32)
            largest = jnp.max(scores, axis=-1, keepdims=True)
            probability = jnp.exp2((scores - largest) * exponent)
            normaliser = jnp.sum(probability, axis=-1, keepdims=True)
            blended = jnp.dot(
                probability.astype(jnp.bfloat16), values, preferred_element_type=jnp.float32)
            results.append(blended / normaliser)
        obuf[k, here] = jnp.where(first, results[0], results[1]).astype(jnp.bfloat16)
        for c in range(CORES):
            to = chip * CORES + lax.rem(core + c, CORES)

            @pl.when(to != s)
            def _():
                out_copy(k, to).start()

            @pl.when(to == s)
            def _():
                out[:, owned_chunk(s, k)] = obuf[k, all_rows_of(s)]

        return 0

    lax.fori_loop(0, len(order), attend_step, 0)

    drain(pbuf.at[pl.ds(0, (2 * chips - 1) * tokens)], p_send.at[0])
    drain(wbuf.at[:, pl.ds(0, 3 * rows)], w_send.at[0])
    drain(kv.at[:, :, pl.ds(0, (n - 1) * tokens)], kv_send.at[0])
    drain(qsend, q_send.at[0])
    drain(obuf.at[:, pl.ds(0, (n - 1) * tokens)], o_send.at[0])
    drain(out.at[:, pl.ds(0, (n - 1) * width)], o_recv.at[0])


def fused_per_device(n, fn, patches, weight_codes, block_scales, key_proj, value_proj, query_gain, key_gain):
    _, tokens, features = patches.shape
    rows, columns = weight_codes.shape
    width = columns // n
    chunks = width // LANES
    group = n // 2 * tokens
    chips = n // 2 // CORES
    bf16 = jnp.bfloat16
    dma = pltpu.SemaphoreType.DMA
    anywhere = pl.BlockSpec(memory_space=pl.ANY)
    result = pl.pallas_call(
        functools.partial(fused_kernel, n, fn),
        out_shape=pltpu.VMEM((tokens, columns), bf16),
        in_specs=[anywhere] * 7,
        out_specs=pl.BlockSpec(memory_space=pltpu.VMEM),
        scratch_shapes=[
            pltpu.VMEM((group, features), bf16),
            pltpu.VMEM((2 * chunks, rows, LANES), jnp.int32),
            pltpu.VMEM((chunks, features, 2 * LANES), bf16),
            pltpu.VMEM((2, tokens, columns), bf16),
            pltpu.VMEM((chunks, 2, n * tokens, LANES), bf16),
            pltpu.VMEM((chunks, group, LANES), bf16),
            pltpu.VMEM((chunks, n * tokens, LANES), bf16),
            pltpu.VMEM((chunks, n * tokens, LANES), bf16),
            pltpu.VMEM((2, 1, columns), jnp.float32),
            pltpu.SMEM(block_scales.shape, jnp.float32),
            dma((2,)), dma((1,)), dma((1,)), dma((1,)), dma((1,)), dma((1,)), dma((1,)), dma((1,)),
            dma((chunks,)), dma((chunks,)), dma((1,)),
            dma((1,)), dma((chunks,)), dma((1,)), dma((chunks,)), dma((1,)), dma((1,)),
            pltpu.SemaphoreType.REGULAR((4,)),
        ],
        compiler_params=pltpu.CompilerParams(
            collective_id=0, has_side_effects=True, vmem_limit_bytes=56 * 1024 * 1024),
    )(
        patches.reshape(tokens, features), weight_codes, block_scales,
        key_proj.reshape(tokens, columns), value_proj.reshape(tokens, columns),
        query_gain.reshape(1, columns), key_gain.reshape(1, columns),
    )
    return result.reshape(1, tokens, columns)


def solution(mesh):
    n, fn = mesh.shape["seq"], mesh.shape["fsdp"]
    specs = (
        P("fsdp", "seq", None), P("fsdp", None), P("fsdp", None),
        P("fsdp", "seq", None), P("fsdp", "seq", None), P(), P(),
    )

    def whole(*arrays):
        patches, weight_codes = arrays[:2]
        fits = patches.shape[0] == fn == GRID * GRID and weight_codes.shape[1] % (n * LANES) == 0 and n == 2 * GRID * CORES
        body = functools.partial(fused_per_device, n, fn) if fits else per_device
        return jax.shard_map(
            body, mesh=mesh, in_specs=specs, out_specs=P("fsdp", "seq", None), check_vma=False
        )(*arrays)

    return whole
```
